32 devices in a mesh: spin: 2 (over x), band: 16 (over z, y, core).
Axes of the slice: x: 2, y: 2, z: 4, core: 2. Of those that a mesh axis runs over, the one named last changes fastest.
Arguments:
- orbitals: bfloat16 [32, 262144], P(('spin', 'band')), parts along dimension 0, may hold values from -6 to 6
- trial: bfloat16 [32, 262144], P(('spin', 'band')), parts along dimension 0, may hold values from -6 to 6
- occupations: int32 [32], P(('spin', 'band')), parts along dimension 0, may hold values 0 or 1
Outputs:
- exchange: bfloat16 [32, 262144], P(('spin', 'band')), parts along dimension 0
- projected: bfloat16 [32, 262144], P('spin', 'band'), parts along dimension 0
The draws below stay inside these ranges and needn't reach their ends.
There are 2 independent parts, one for each index of `spin`. The reference program is written for one: setup_inputs(seed, part) draws one part's arguments, and reference() takes and returns one part's arrays. A program takes and returns all parts, laid end to end along the dimension named above; each array names one. Nothing has to cross between parts.
All inputs are finite; a program needn't handle non-finite values. No bound on the sum of `occupations` on one device may be relied on, other than what follows from the above.
Results may differ from the reference program's by a relative error of at most 0.018.
Values may be sent and summed in bfloat16 or wider, within the bound.
A program may use at most 64 MiB of HBM per device.

```python
import math
import jax
import jax.numpy as jnp
from jax import lax

NG = 64
ORB_DEV = 1
SHIFTS = 1
G = 262144
ORBITALS = 16
N_BAND = 16


def touch_ends(values, stream_key, smallest, high):
    longest = values.shape.index(max(values.shape))
    spots = []
    for shift in (0, 1):
        where = [jax.random.randint(jax.random.fold_in(stream_key, axis), (), 0, length) for axis, length in enumerate(values.shape)]
        where[longest] = (where[longest] + shift) % values.shape[longest]
        spots.append(tuple(where))
    return values.at[spots[0]].set(smallest).at[spots[1]].set(high)


def block_levels(rng, shape, shards, smallest, top_value):
    level, own = 1.0, jax.random.fold_in(rng, 6)
    for position, blocks in shards:
        draws = jnp.exp(jax.random.uniform(jax.random.fold_in(own, position), (blocks,), jnp.float32, smallest / len(shards), top_value / len(shards)))
        level = level * jnp.repeat(draws, shape[position] // blocks).reshape([-1 if axis == position else 1 for axis in range(len(shape))])
    return level


def bell_draw(stream_key, shape, scale, reach, pieces=(), held_as=jnp.bfloat16):
    array = jax.random.normal(stream_key, shape, jnp.float32) * scale
    if len(pieces) > 0:
        array = block_levels(stream_key, shape, pieces, -0.22, 0.18) * array
    return jnp.clip(array, min=-reach, max=reach).astype(held_as)


def setup_inputs(seed: int = 0, part: int = 0) -> dict:
    keys = jax.random.split(jax.random.key(seed), 4)
    own_keys = jax.random.split(jax.random.fold_in(keys[3], part), 4)
    return {
        "orbitals": bell_draw(own_keys[0], (ORBITALS, G), 1.0, 6.0, ((0, 16),)),
        "trial": bell_draw(own_keys[1], (ORBITALS, G), 1.0, 6.0, ((0, 16),)),
        "occupations": touch_ends((jax.random.randint(own_keys[2], (ORBITALS,), 0, 4) < 3).astype(jnp.int32), jax.random.fold_in(own_keys[2], 1), 0, 1),
    }


FRACTION = 0.25
OMEGA = 1.0

def cas_table(extent):
    indices = jnp.arange(extent, dtype=jnp.int32)
    products = indices[:, None] * indices[None, :] % extent
    phases = products.astype(jnp.float32) * (2.0 * math.pi / extent)
    return (jnp.cos(phases) + jnp.sin(phases)).astype(jnp.bfloat16)

def screened_kernel(extent):
    modes = jnp.arange(extent, dtype=jnp.int32)
    modes = jnp.where(2 * modes < extent, modes, modes - extent)
    wavenum = modes.astype(jnp.float32) * (2.0 * math.pi / extent)
    squares = wavenum * wavenum
    norm_sq = squares[:, None, None] + squares[None, :, None] + squares[None, None, :]
    bounded = jnp.where(norm_sq > 0, norm_sq, 1.0)
    screened = jnp.where(norm_sq > 0, 4.0 * math.pi / bounded * (1.0 - jnp.exp(-bounded / (4.0 * OMEGA * OMEGA))), math.pi / (OMEGA * OMEGA))
    return (screened / extent ** 3).reshape(-1)

def sweep(values, pattern, table):
    rounded = lax.optimization_barrier(values)
    return jnp.einsum(pattern, table.astype(jnp.float32), rounded.astype(jnp.float32), precision=lax.Precision.HIGHEST)

def screened_potential(density, table, kernel, extent):
    number = density.shape[0]
    values = density.reshape(number, extent, extent, extent)
    patterns = ('ga,pabc->pgbc', 'gb,pabc->pagc', 'gc,pabc->pabg')
    for pattern in patterns:
        values = sweep(values, pattern, table).astype(jnp.bfloat16)
    values = lax.optimization_barrier(values)
    values = (values.astype(jnp.float32) * kernel.reshape(extent, extent, extent)).astype(jnp.bfloat16)
    for ordinal, pattern in enumerate(patterns):
        values = sweep(values, pattern, table)
        if ordinal < 2:
            values = values.astype(jnp.bfloat16)
    return values.reshape(number, -1)

def reference(orbitals, trial, occupations):
    table = cas_table(NG)
    kernel = screened_kernel(NG)
    blocks = orbitals.reshape(N_BAND, ORB_DEV, G)
    fills = occupations.astype(jnp.float32).reshape(N_BAND, ORB_DEV)

    def one_block(block_index):
        own = lax.dynamic_index_in_dim(blocks, block_index, 0, keepdims=False)
        accumulated = jnp.zeros((ORB_DEV, G), jnp.float32)
        for offset in range(-SHIFTS, SHIFTS + 1):
            partner = ((block_index - offset) % N_BAND).astype(jnp.int32)
            visitors = lax.dynamic_index_in_dim(blocks, partner, 0, keepdims=False)
            partner_fill = lax.dynamic_index_in_dim(fills, partner, 0, keepdims=False)
            density = (own[:, None, :].astype(jnp.float32) * visitors[None, :, :].astype(jnp.float32)).astype(jnp.bfloat16)
            potential = screened_potential(density.reshape(ORB_DEV * ORB_DEV, G), table, kernel, NG).reshape(ORB_DEV, ORB_DEV, G)
            accumulated = accumulated + jnp.einsum('ijg,j,jg->ig', potential, partner_fill, visitors.astype(jnp.float32), precision=lax.Precision.HIGHEST)
        return (-FRACTION * accumulated).astype(jnp.bfloat16)
    exchange = lax.map(one_block, jnp.arange(N_BAND, dtype=jnp.int32)).reshape(ORBITALS, G)
    intersection = lax.dot_general(exchange, trial, (((1,), (1,)), ((), ())), preferred_element_type=jnp.float32) / math.sqrt(G)
    intersection_low = intersection.astype(jnp.bfloat16)
    projected = -(lax.dot_general(intersection_low, exchange, (((0,), (0,)), ((), ())), preferred_element_type=jnp.float32) / math.sqrt(ORBITALS))
    return (exchange, projected.astype(jnp.bfloat16))
```

```python
import functools
import math

import jax
import jax.numpy as jnp
import numpy as np
from jax import lax
from jax.experimental import pallas as pl
from jax.experimental.pallas import tpu as pltpu
from jax.sharding import PartitionSpec as P

NG = 64
FRACTION = 0.25
OMEGA = 1.0
LANES = 128
TILE = 256
CHUNKS = 4
MESH = pl.DeviceIdType.MESH

HALF = NG // 2
PLANE = NG * NG
ROWS = NG * NG * NG // LANES


def cas_table():
    index = np.arange(NG)
    phases = (index[:, None] * index[None, :] % NG).astype(np.float32) * np.float32(2.0 * math.pi / NG)
    return np.cos(phases) + np.sin(phases)


def tables():
    table = cas_table()
    order = np.concatenate([np.arange(0, NG, 2), np.arange(1, NG, 2)])
    eye = np.eye(TILE // NG, dtype=np.float32)
    left_a = np.kron(eye, table)
    left_b = np.kron(eye, table[order][:, order])
    right_c = np.kron(np.eye(LANES // NG, dtype=np.float32), table)
    return [jnp.asarray(t).astype(jnp.bfloat16) for t in (left_a, left_b, right_c)]


def dot(left, right):
    return jnp.dot(left, right, preferred_element_type=jnp.float32)


def low(value):
    return value.astype(jnp.bfloat16)


def wide(value):
    return value.astype(jnp.float32)


def exchanged(first, second):
    lower = lax.broadcasted_iota(jnp.int32, first.shape, 1) < LANES // 2
    return (
        jnp.where(lower, first, pltpu.roll(second, LANES // 2, 1)),
        jnp.where(lower, pltpu.roll(first, LANES // 2, 1), second),
    )


def wavenum_sq(index):
    modes = wide(jnp.where(2 * index < NG, index, index - NG))
    wavenum = modes * (2.0 * math.pi / NG)
    return wavenum * wavenum


def screened_rows(group):
    shape = (TILE, LANES)
    row = lax.broadcasted_iota(jnp.int32, shape, 0)
    lane = lax.broadcasted_iota(jnp.int32, shape, 1)
    a = row % NG
    b = 2 * (group * (TILE // NG) + row // NG) + lane // NG
    norm_sq = wavenum_sq(a) + wavenum_sq(b) + wavenum_sq(lane % NG)
    bounded = jnp.where(norm_sq > 0, norm_sq, 1.0)
    screened = jnp.where(
        norm_sq > 0,
        4.0 * math.pi / bounded * (1.0 - jnp.exp(-bounded / (4.0 * OMEGA * OMEGA))),
        math.pi / (OMEGA * OMEGA),
    )
    return screened * (1.0 / NG**3)


def partner(me, step, count):
    total, bit = 0, 1
    while bit < count:
        total = total + bit * ((me // bit + step // bit) % 2)
        bit *= 2
    return total


def body(
    count,
    orb_hbm, tri_hbm, occ, left_a, left_b, right_c,
    exch_hbm, proj_hbm,
    orb_line, tri_line, own, own_w, sibling, remote, tri_rows, kern, field, acc,
    e_rows, t_in, e_in, tt, et, part, parts, exch_line, proj,
    load_sem, orb_send, orb_recv, t_send, t_recv, e_send, e_recv, p_send, p_recv, out_sem,
):
    me = lax.axis_index("band")
    barrier = pltpu.get_barrier_semaphore()
    slab = ROWS // count
    pack = TILE // count
    spread = LANES // count
    groups = slab // pack
    tiles = ROWS // TILE
    per_tile = TILE // NG

    load_orb = pltpu.make_async_copy(orb_hbm, orb_line, load_sem.at[0])
    load_tri = pltpu.make_async_copy(tri_hbm, tri_line, load_sem.at[1])
    load_orb.start()
    load_tri.start()

    @pl.loop(1, count)
    def _(step):
        pl.semaphore_signal(
            barrier, inc=1, device_id={"band": partner(me, step, count)}, device_id_type=MESH
        )

    def plane(ref, a):
        cut = pl.ds(pl.multiple_of(a * PLANE, PLANE), PLANE)
        return wide(ref[:, cut]).reshape(PLANE // LANES, LANES)

    fill = occ[0].astype(jnp.float32)
    load_orb.wait()

    @pl.loop(0, HALF)
    def _(a):
        pair = jnp.concatenate(exchanged(plane(orb_line, a), plane(orb_line, a + HALF)), axis=0)
        cut = pl.ds(pl.multiple_of(a * NG, NG), NG)
        own[cut, :] = low(pair)
        own_w[cut, :] = low(pair * fill)

    load_tri.wait()
    flat_rows = tri_rows.reshape(ROWS, LANES)

    @pl.loop(0, NG)
    def _(a):
        flat_rows[pl.ds(pl.multiple_of(a * (PLANE // LANES), PLANE // LANES), PLANE // LANES), :] = low(
            plane(tri_line, a)
        )

    sib = me + 1 - 2 * (me % 2)
    rem = (me + count - 1 + 2 * (me % 2)) % count
    depth = ROWS // CHUNKS

    def orbital(side, chunk):
        cut = pl.ds(chunk * depth, depth)
        return pltpu.make_async_remote_copy(
            src_ref=own_w.at[cut],
            dst_ref=(sibling, remote)[side].at[cut],
            send_sem=orb_send.at[side, chunk],
            recv_sem=orb_recv.at[side, chunk],
            device_id={"band": (sib, rem)[side]},
            device_id_type=MESH,
        )

    def slab_copy(src, dst, send, recv, peer, slot):
        return pltpu.make_async_remote_copy(
            src_ref=src,
            dst_ref=dst.at[slot],
            send_sem=send.at[peer],
            recv_sem=recv.at[slot],
            device_id={"band": peer},
            device_id_type=MESH,
        )

    def trial_copy(peer, slot):
        return slab_copy(tri_rows.at[peer], t_in, t_send, t_recv, peer, slot)

    def exchange_copy(peer, slot):
        return slab_copy(e_rows.at[peer], e_in, e_send, e_recv, peer, slot)

    def part_copy(peer, slot):
        return slab_copy(part, parts, p_send, p_recv, peer, slot)

    pl.semaphore_wait(barrier, count - 1)
    for chunk in range(CHUNKS):
        orbital(1, chunk).start()
    for chunk in range(CHUNKS):
        orbital(0, chunk).start()

    def send_trial(low_bits):
        @pl.loop(0, count // 4)
        def _(i):
            for bits in low_bits:
                step = (count // 4 - 1 - i) * 4 + bits
                peer = partner(me, step, count)
                if bits == 0:

                    @pl.when(i < count // 4 - 1)
                    def _():
                        trial_copy(peer, me).start()
                else:
                    trial_copy(peer, me).start()

    send_trial((0, 1))

    @pl.loop(0, tiles)
    def _(group):
        kern[pl.ds(pl.multiple_of(group * TILE, TILE), TILE), :] = screened_rows(group)

    def tile(group):
        return pl.ds(pl.multiple_of(group * TILE, TILE), TILE)

    def rise(weighted, start, stop):
        @pl.loop(start, stop)
        def _(group):
            cut = tile(group)
            density = low(wide(own[cut, :]) * wide(weighted[cut, :]))
            field[cut, :] = dot(left_b[...], low(dot(density, right_c[...])))

    def turn():
        @pl.loop(0, tiles)
        def _(group):
            pieces = []
            for j in range(per_tile):
                b = group * per_tile + j
                pieces += exchanged(
                    field[pl.ds(b, HALF, stride=NG), :], field[pl.ds(b + HALF, HALF, stride=NG), :]
                )
            value = low(dot(left_a[...], low(jnp.concatenate(pieces, axis=0))))
            value = low(wide(value) * kern[tile(group), :])
            value = low(dot(left_a[...], value))
            value = dot(value, right_c[...])
            for j in range(per_tile):
                b = group * per_tile + j
                first, second = exchanged(
                    value[j * NG : j * NG + HALF], value[j * NG + HALF : (j + 1) * NG]
                )
                field[pl.ds(b, HALF, stride=NG), :] = first
                field[pl.ds(b + HALF, HALF, stride=NG), :] = second

    def fall(weighted, group):
        cut = tile(group)
        return dot(left_b[...], low(field[cut, :])) * wide(weighted[cut, :])

    rise(own_w, 0, tiles)
    turn()

    @pl.loop(0, tiles)
    def _(group):
        acc[tile(group), :] = fall(own_w, group)

    for chunk in range(CHUNKS):
        orbital(0, chunk).wait_recv()
    rise(sibling, 0, tiles)
    turn()

    @pl.loop(0, tiles)
    def _(group):
        acc[tile(group), :] += fall(sibling, group)

    for chunk in range(CHUNKS):
        orbital(1, chunk).wait_recv()
        rise(remote, chunk * tiles // CHUNKS, (chunk + 1) * tiles // CHUNKS)
    send_trial((2, 3))
    turn()
    flat_e = e_rows.reshape(ROWS, LANES)

    @pl.loop(0, tiles)
    def _(group):
        value = -FRACTION * (acc[tile(group), :] + fall(remote, group))
        for j in range(per_tile):
            a = group * per_tile + j
            first, second = exchanged(
                value[j * NG : j * NG + HALF], value[j * NG + HALF : (j + 1) * NG]
            )
            flat_e[pl.ds(pl.multiple_of(a * HALF, HALF), HALF), :] = low(first)
            flat_e[pl.ds(pl.multiple_of((a + HALF) * HALF, HALF), HALF), :] = low(second)

    t_in[pl.ds(me, 1)] = tri_rows[pl.ds(me, 1)]
    e_in[pl.ds(me, 1)] = e_rows[pl.ds(me, 1)]

    @pl.loop(1, count)
    def _(i):
        peer = partner(me, count - i, count)
        exchange_copy(peer, me).start()

    @pl.loop(0, NG)
    def _(a):
        cut = pl.ds(pl.multiple_of(a * PLANE, PLANE), PLANE)
        rows = wide(flat_e[pl.ds(pl.multiple_of(a * HALF, HALF), HALF), :])
        exch_line[:, cut] = low(rows.reshape(1, PLANE))

    store_exch = pltpu.make_async_copy(exch_line, exch_hbm, out_sem.at[0])
    store_exch.start()

    def spread_out(src, dst, slot):
        dst[pl.ds(slot, slab, stride=count), :] = wide(src[slot])

    spread_out(t_in, tt, me)

    @pl.loop(1, count)
    def _(i):
        peer = partner(me, count - i, count)
        trial_copy(peer, peer).wait_recv()
        spread_out(t_in, tt, peer)

    spread_out(e_in, et, me)

    @pl.loop(1, count)
    def _(i):
        peer = partner(me, i, count)
        exchange_copy(peer, peer).wait_recv()
        spread_out(e_in, et, peer)

    def side_by_side(ref):
        return jnp.concatenate([low(ref[g * TILE : (g + 1) * TILE, :]) for g in range(groups)], axis=1)

    gram = lax.dot_general(
        side_by_side(tt), side_by_side(et), (((1,), (1,)), ((), ())), preferred_element_type=jnp.float32
    )
    column = lax.broadcasted_iota(jnp.int32, (count, TILE), 1) // count
    total = jnp.zeros((count, TILE), jnp.float32)
    for r in range(pack):
        total = total + jnp.where(column == r, gram[r * count : (r + 1) * count], 0.0)
    total = total[:, :LANES] + total[:, LANES:]
    shift = LANES // 2
    while shift >= count:
        total = total + pltpu.roll(total, shift, 1)
        shift //= 2
    here = (
        lax.broadcasted_iota(jnp.int32, (count, LANES), 0) % spread
        == lax.broadcasted_iota(jnp.int32, (count, LANES), 1) // count
    )
    if spread > 1:
        total = jnp.sum(
            jnp.where(here, total, 0.0).reshape(count // spread, spread, LANES), axis=1
        )
    part[...] = total
    parts[pl.ds(me, 1)] = total[None]

    @pl.loop(1, count)
    def _(i):
        part_copy(partner(me, count - i, count), me).start()

    @pl.loop(1, count)
    def _(i):
        peer = partner(me, i, count)
        part_copy(peer, peer).wait_recv()

    total = jnp.sum(parts[...], axis=0) / math.sqrt(ROWS * LANES)
    if spread > 1:
        total = jnp.broadcast_to(total[:, None, :], (count // spread, spread, LANES)).reshape(
            count, LANES
        )
        total = jnp.where(here, total, 0.0)
        shift = LANES // 2
        while shift >= count:
            total = total + pltpu.roll(total, shift, 1)
            shift //= 2
    total = jnp.concatenate([total, total], axis=1)
    mixing = low(
        jnp.concatenate([jnp.where(column == r, total, 0.0) for r in range(pack)], axis=0)
    )
    for group in range(groups):
        piece = dot(mixing, low(et[group * TILE : (group + 1) * TILE, :]))
        piece = low(piece * (-1.0 / math.sqrt(count)))
        for r in range(pack):
            at = (group * pack + r) * LANES
            proj[:, at : at + LANES] = piece[r * count : (r + 1) * count]
    store_proj = pltpu.make_async_copy(proj, proj_hbm, out_sem.at[1])
    store_proj.start()

    for chunk in range(CHUNKS):
        for side in range(2):
            orbital(side, chunk).wait_send()

    @pl.loop(1, count)
    def _(i):
        peer = partner(me, i, count)
        trial_copy(peer, me).wait_send()
        exchange_copy(peer, me).wait_send()
        part_copy(peer, me).wait_send()

    store_exch.wait()
    store_proj.wait()


def local(orbitals, trial, occupations):
    count = lax.axis_size("band")
    cells = orbitals.shape[1]
    slab = ROWS // count
    rows = (ROWS, LANES)
    bf16, f32 = jnp.bfloat16, jnp.float32
    spread = LANES // count
    compact = (count // spread, LANES)
    dma = pltpu.SemaphoreType.DMA
    anywhere = pl.BlockSpec(memory_space=pl.ANY)
    vmem = pl.BlockSpec(memory_space=pltpu.VMEM)
    return pl.pallas_call(
        functools.partial(body, count),
        out_shape=(
            jax.ShapeDtypeStruct((1, cells), bf16),
            jax.ShapeDtypeStruct((count, cells // count), bf16),
        ),
        in_specs=[anywhere, anywhere, pl.BlockSpec(memory_space=pltpu.SMEM), vmem, vmem, vmem],
        out_specs=(anywhere, anywhere),
        scratch_shapes=[
            pltpu.VMEM((1, cells), bf16),
            pltpu.VMEM((1, cells), bf16),
            pltpu.VMEM(rows, bf16),
            pltpu.VMEM(rows, bf16),
            pltpu.VMEM(rows, bf16),
            pltpu.VMEM(rows, bf16),
            pltpu.VMEM((count, slab, LANES), bf16),
            pltpu.VMEM(rows, f32),
            pltpu.VMEM(rows, f32),
            pltpu.VMEM(rows, f32),
            pltpu.VMEM((count, slab, LANES), bf16),
            pltpu.VMEM((count, slab, LANES), bf16),
            pltpu.VMEM((count, slab, LANES), bf16),
            pltpu.VMEM(rows, f32),
            pltpu.VMEM(rows, f32),
            pltpu.VMEM(compact, f32),
            pltpu.VMEM((count,) + compact, f32),
            pltpu.VMEM((1, cells), bf16),
            pltpu.VMEM((count, cells // count), bf16),
            dma((2,)),
            dma((2, CHUNKS)),
            dma((2, CHUNKS)),
            dma((count,)),
            dma((count,)),
            dma((count,)),
            dma((count,)),
            dma((count,)),
            dma((count,)),
            dma((2,)),
        ],
        compiler_params=pltpu.CompilerParams(collective_id=1, has_side_effects=True),
        name="exchange_and_projection",
    )(orbitals, trial, occupations, *tables())


def solution(mesh):
    return jax.shard_map(
        local,
        mesh=mesh,
        in_specs=(P(("spin", "band"), None), P(("spin", "band"), None), P(("spin", "band"))),
        out_specs=(P(("spin", "band"), None), P("spin", "band")),
        check_vma=False,
    )
```

```python
import functools
import math

import jax
import jax.numpy as jnp
import numpy as np
from jax import lax
from jax.experimental import pallas as pl
from jax.experimental.pallas import tpu as pltpu
from jax.sharding import PartitionSpec as P

NG = 64
FRACTION = 0.25
OMEGA = 1.0
LANES = 128
TILE = 256
CHUNKS = 4
UNROLL = 2
MESH = pl.DeviceIdType.MESH

HALF = NG // 2
SUB = TILE // HALF
PLANE = NG * NG
ROWS = NG * NG * NG // LANES


def cas_table():
    index = np.arange(NG)
    phases = (index[:, None] * index[None, :] % NG).astype(np.float32) * np.float32(2.0 * math.pi / NG)
    return np.cos(phases) + np.sin(phases)


def tables():
    table = cas_table()
    order = np.concatenate([np.arange(0, NG, 2), np.arange(1, NG, 2)])
    eye = np.eye(TILE // NG, dtype=np.float32)
    sums = np.array([[1.0, 1.0], [1.0, -1.0]], np.float32)
    right_c = np.kron(np.eye(TILE // LANES, dtype=np.float32), np.kron(sums, table))
    left_b = np.kron(eye, table[order][:, order])
    halves = (table[0::2, :HALF], table[1::2, :HALF])
    rows = np.eye(TILE // HALF, dtype=np.float32)
    left_a = np.concatenate([np.kron(half, rows) for half in halves])
    back_a = np.concatenate([np.kron(half.T, rows) for half in halves])
    return [jnp.asarray(t).astype(jnp.bfloat16) for t in (left_a, back_a, left_b, right_c)]


def dot(left, right):
    return jnp.dot(left, right, preferred_element_type=jnp.float32)


def low(value):
    return value.astype(jnp.bfloat16)


def wide(value):
    return value.astype(jnp.float32)


def exchanged(first, second):
    lower = lax.broadcasted_iota(jnp.int32, first.shape, 1) < LANES // 2
    return (
        jnp.where(lower, first, pltpu.roll(second, LANES // 2, 1)),
        jnp.where(lower, pltpu.roll(first, LANES // 2, 1), second),
    )


def wavenum_sq(index):
    modes = wide(jnp.where(2 * index < NG, index, index - NG))
    wavenum = modes * (2.0 * math.pi / NG)
    return wavenum * wavenum


def screened_rows(group):
    shape = (TILE, LANES)
    row = lax.broadcasted_iota(jnp.int32, shape, 0)
    lane = lax.broadcasted_iota(jnp.int32, shape, 1)
    a = 2 * (row // SUB) + lane // NG
    place = group * SUB + row % SUB
    b = 2 * (place % HALF) + place // HALF
    norm_sq = wavenum_sq(a) + wavenum_sq(b) + wavenum_sq(lane % NG)
    bounded = jnp.where(norm_sq > 0, norm_sq, 1.0)
    screened = jnp.where(
        norm_sq > 0,
        4.0 * math.pi / bounded * (1.0 - jnp.exp(-bounded / (4.0 * OMEGA * OMEGA))),
        math.pi / (OMEGA * OMEGA),
    )
    return screened * (1.0 / NG**3)


def partner(me, step, count):
    total, bit = 0, 1
    while bit < count:
        total = total + bit * ((me // bit + step // bit) % 2)
        bit *= 2
    return total


def body(
    count,
    orb_hbm, tri_hbm, occ, left_a, back_a, left_b, right_c,
    exch_hbm, proj_hbm,
    orb_line, tri_line, own, own_w, sibling, remote, tri_rows, kern, field, acc,
    e_rows, t_in, e_in, tt, et, part, parts, exch_line, proj,
    load_sem, orb_send, orb_recv, t_send, t_recv, e_send, e_recv, p_send, p_recv, out_sem,
):
    me = lax.axis_index("band")
    barrier = pltpu.get_barrier_semaphore()
    slab = ROWS // count
    pack = TILE // count
    spread = LANES // count
    groups = slab // pack
    tiles = ROWS // TILE
    per_tile = TILE // NG

    load_orb = pltpu.make_async_copy(orb_hbm, orb_line, load_sem.at[0])
    load_tri = pltpu.make_async_copy(tri_hbm, tri_line, load_sem.at[1])
    load_orb.start()
    load_tri.start()

    @pl.loop(1, count)
    def _(step):
        pl.semaphore_signal(
            barrier, inc=1, device_id={"band": partner(me, step, count)}, device_id_type=MESH
        )

    def plane(ref, a):
        cut = pl.ds(pl.multiple_of(a * PLANE, PLANE), PLANE)
        return wide(ref[:, cut]).reshape(PLANE // LANES, LANES)

    fill = occ[0].astype(jnp.float32)
    load_orb.wait()

    @pl.loop(0, HALF)
    def _(a):
        pair = jnp.concatenate(exchanged(plane(orb_line, a), plane(orb_line, a + HALF)), axis=0)
        cut = pl.ds(pl.multiple_of(a * NG, NG), NG)
        own[cut, :] = low(pair)
        own_w[cut, :] = low(pair * fill)

    flat_rows = tri_rows.reshape(ROWS, LANES)
    load_tri.wait()

    @pl.loop(0, NG)
    def _(a):
        flat_rows[pl.ds(pl.multiple_of(a * (PLANE // LANES), PLANE // LANES), PLANE // LANES), :] = low(
            plane(tri_line, a)
        )

    sib = me + 1 - 2 * (me % 2)
    rem = (me + count - 1 + 2 * (me % 2)) % count
    depth = ROWS // CHUNKS

    def orbital(side, chunk):
        cut = pl.ds(chunk * depth, depth)
        return pltpu.make_async_remote_copy(
            src_ref=own_w.at[cut],
            dst_ref=(sibling, remote)[side].at[cut],
            send_sem=orb_send.at[side, chunk],
            recv_sem=orb_recv.at[side, chunk],
            device_id={"band": (sib, rem)[side]},
            device_id_type=MESH,
        )

    def slab_copy(src, dst, send, recv, peer, slot):
        return pltpu.make_async_remote_copy(
            src_ref=src,
            dst_ref=dst.at[slot],
            send_sem=send.at[peer],
            recv_sem=recv.at[slot],
            device_id={"band": peer},
            device_id_type=MESH,
        )

    def trial_copy(peer, slot):
        return slab_copy(tri_rows.at[peer], t_in, t_send, t_recv, peer, slot)

    def exchange_copy(peer, slot):
        return slab_copy(e_rows.at[peer], e_in, e_send, e_recv, peer, slot)

    def part_copy(peer, slot):
        return slab_copy(part, parts, p_send, p_recv, peer, slot)

    pl.semaphore_wait(barrier, count - 1)
    for chunk in range(CHUNKS):
        orbital(1, chunk).start()
    for chunk in range(CHUNKS):
        orbital(0, chunk).start()

    def send_trial(low_bits):
        @pl.loop(0, count // 4)
        def _(i):
            for bits in low_bits:
                step = (count // 4 - 1 - i) * 4 + bits
                peer = partner(me, step, count)
                if bits == 0:

                    @pl.when(i < count // 4 - 1)
                    def _():
                        trial_copy(peer, me).start()
                else:
                    trial_copy(peer, me).start()

    send_trial((0, 1))

    @pl.loop(0, tiles)
    def _(group):
        kern[pl.ds(pl.multiple_of(group * TILE, TILE), TILE), :] = screened_rows(group)

    def tile(group):
        return pl.ds(pl.multiple_of(group * TILE, TILE), TILE)

    def two(read, step):
        return jnp.concatenate([read(2 * step), read(2 * step + 1)], axis=1)

    def halved(value):
        lane = lax.broadcasted_iota(jnp.int32, (TILE, TILE), 1)
        return jnp.where(lane % LANES < LANES // 2, value[:TILE], value[TILE:])

    def rise(weighted, start, stop):
        @pl.loop(start // 2, stop // 2, unroll=min(UNROLL, (stop - start) // 2))
        def _(step):
            density = two(
                lambda group: low(wide(own[tile(group), :]) * wide(weighted[tile(group), :])), step
            )
            value = dot(left_b[...], low(dot(density, right_c[...])))
            field[tile(2 * step), :] = value[:, :LANES]
            field[tile(2 * step + 1), :] = value[:, LANES:]

    def strip(a, group):
        return pl.ds(pl.multiple_of(a * NG + group * SUB, SUB), SUB)

    def turn():
        @pl.loop(0, tiles // 2, unroll=UNROLL)
        def _(step):
            value = two(
                lambda group: low(
                    jnp.concatenate([field[strip(a, group), :] for a in range(HALF)], axis=0)
                ),
                step,
            )
            value = low(halved(dot(left_a[...], value)))
            value = low(wide(value) * two(lambda group: kern[tile(group), :], step))
            value = low(halved(dot(back_a[...], value)))
            value = dot(value, right_c[...])
            for side in range(2):
                for a in range(HALF):
                    field[strip(a, 2 * step + side), :] = value[
                        a * SUB : (a + 1) * SUB, side * LANES : (side + 1) * LANES
                    ]

    def fall(weighted, step):
        value = dot(left_b[...], two(lambda group: low(field[tile(group), :]), step))
        return [
            value[:, side * LANES : (side + 1) * LANES] * wide(weighted[tile(2 * step + side), :])
            for side in range(2)
        ]

    rise(own_w, 0, tiles)
    turn()

    @pl.loop(0, tiles // 2, unroll=UNROLL)
    def _(step):
        for side, value in enumerate(fall(own_w, step)):
            acc[tile(2 * step + side), :] = value

    for chunk in range(CHUNKS):
        orbital(0, chunk).wait_recv()
    rise(sibling, 0, tiles)
    turn()

    @pl.loop(0, tiles // 2, unroll=UNROLL)
    def _(step):
        for side, value in enumerate(fall(sibling, step)):
            acc[tile(2 * step + side), :] += value

    for chunk in range(CHUNKS):
        orbital(1, chunk).wait_recv()
        rise(remote, chunk * tiles // CHUNKS, (chunk + 1) * tiles // CHUNKS)
    send_trial((2, 3))
    turn()
    flat_e = e_rows.reshape(ROWS, LANES)

    @pl.loop(0, tiles // 2, unroll=UNROLL)
    def _(step):
        for side, value in enumerate(fall(remote, step)):
            group = 2 * step + side
            value = -FRACTION * (acc[tile(group), :] + value)
            for j in range(per_tile):
                a = group * per_tile + j
                first, second = exchanged(
                    value[j * NG : j * NG + HALF], value[j * NG + HALF : (j + 1) * NG]
                )
                flat_e[pl.ds(pl.multiple_of(a * HALF, HALF), HALF), :] = low(first)
                flat_e[pl.ds(pl.multiple_of((a + HALF) * HALF, HALF), HALF), :] = low(second)

    t_in[pl.ds(me, 1)] = tri_rows[pl.ds(me, 1)]
    e_in[pl.ds(me, 1)] = e_rows[pl.ds(me, 1)]

    @pl.loop(1, count)
    def _(i):
        peer = partner(me, count - i, count)
        exchange_copy(peer, me).start()

    @pl.loop(0, NG)
    def _(a):
        cut = pl.ds(pl.multiple_of(a * PLANE, PLANE), PLANE)
        rows = wide(flat_e[pl.ds(pl.multiple_of(a * HALF, HALF), HALF), :])
        exch_line[:, cut] = low(rows.reshape(1, PLANE))

    store_exch = pltpu.make_async_copy(exch_line, exch_hbm, out_sem.at[0])
    store_exch.start()

    def spread_out(src, dst, slot):
        dst[pl.ds(slot, slab, stride=count), :] = wide(src[slot])

    spread_out(t_in, tt, me)

    @pl.loop(1, count)
    def _(i):
        peer = partner(me, count - i, count)
        trial_copy(peer, peer).wait_recv()
        spread_out(t_in, tt, peer)

    spread_out(e_in, et, me)

    @pl.loop(1, count)
    def _(i):
        peer = partner(me, i, count)
        exchange_copy(peer, peer).wait_recv()
        spread_out(e_in, et, peer)

    def side_by_side(ref):
        return jnp.concatenate([low(ref[g * TILE : (g + 1) * TILE, :]) for g in range(groups)], axis=1)

    gram = lax.dot_general(
        side_by_side(tt), side_by_side(et), (((1,), (1,)), ((), ())), preferred_element_type=jnp.float32
    )
    column = lax.broadcasted_iota(jnp.int32, (count, TILE), 1) // count
    total = jnp.zeros((count, TILE), jnp.float32)
    for r in range(pack):
        total = total + jnp.where(column == r, gram[r * count : (r + 1) * count], 0.0)
    total = total[:, :LANES] + total[:, LANES:]
    shift = LANES // 2
    while shift >= count:
        total = total + pltpu.roll(total, shift, 1)
        shift //= 2
    here = (
        lax.broadcasted_iota(jnp.int32, (count, LANES), 0) % spread
        == lax.broadcasted_iota(jnp.int32, (count, LANES), 1) // count
    )
    if spread > 1:
        total = jnp.sum(
            jnp.where(here, total, 0.0).reshape(count // spread, spread, LANES), axis=1
        )
    part[...] = total
    parts[pl.ds(me, 1)] = total[None]

    @pl.loop(1, count)
    def _(i):
        part_copy(partner(me, count - i, count), me).start()

    @pl.loop(1, count)
    def _(i):
        peer = partner(me, i, count)
        part_copy(peer, peer).wait_recv()

    total = jnp.sum(parts[...], axis=0) / math.sqrt(ROWS * LANES)
    if spread > 1:
        total = jnp.broadcast_to(total[:, None, :], (count // spread, spread, LANES)).reshape(
            count, LANES
        )
        total = jnp.where(here, total, 0.0)
        shift = LANES // 2
        while shift >= count:
            total = total + pltpu.roll(total, shift, 1)
            shift //= 2
    total = jnp.concatenate([total, total], axis=1)
    mixing = low(
        jnp.concatenate([jnp.where(column == r, total, 0.0) for r in range(pack)], axis=0)
    )
    for group in range(groups):
        piece = dot(mixing, low(et[group * TILE : (group + 1) * TILE, :]))
        piece = low(piece * (-1.0 / math.sqrt(count)))
        for r in range(pack):
            at = (group * pack + r) * LANES
            proj[:, at : at + LANES] = piece[r * count : (r + 1) * count]
    store_proj = pltpu.make_async_copy(proj, proj_hbm, out_sem.at[1])
    store_proj.start()

    for chunk in range(CHUNKS):
        for side in range(2):
            orbital(side, chunk).wait_send()

    @pl.loop(1, count)
    def _(i):
        peer = partner(me, i, count)
        trial_copy(peer, me).wait_send()
        exchange_copy(peer, me).wait_send()
        part_copy(peer, me).wait_send()

    store_exch.wait()
    store_proj.wait()


def local(orbitals, trial, occupations):
    count = lax.axis_size("band")
    cells = orbitals.shape[1]
    slab = ROWS // count
    rows = (ROWS, LANES)
    bf16, f32 = jnp.bfloat16, jnp.float32
    spread = LANES // count
    compact = (count // spread, LANES)
    dma = pltpu.SemaphoreType.DMA
    anywhere = pl.BlockSpec(memory_space=pl.ANY)
    vmem = pl.BlockSpec(memory_space=pltpu.VMEM)
    return pl.pallas_call(
        functools.partial(body, count),
        out_shape=(
            jax.ShapeDtypeStruct((1, cells), bf16),
            jax.ShapeDtypeStruct((count, cells // count), bf16),
        ),
        in_specs=[anywhere, anywhere, pl.BlockSpec(memory_space=pltpu.SMEM), vmem, vmem, vmem, vmem],
        out_specs=(anywhere, anywhere),
        scratch_shapes=[
            pltpu.VMEM((1, cells), bf16),
            pltpu.VMEM((1, cells), bf16),
            pltpu.VMEM(rows, bf16),
            pltpu.VMEM(rows, bf16),
            pltpu.VMEM(rows, bf16),
            pltpu.VMEM(rows, bf16),
            pltpu.VMEM((count, slab, LANES), bf16),
            pltpu.VMEM(rows, f32),
            pltpu.VMEM(rows, f32),
            pltpu.VMEM(rows, f32),
            pltpu.VMEM((count, slab, LANES), bf16),
            pltpu.VMEM((count, slab, LANES), bf16),
            pltpu.VMEM((count, slab, LANES), bf16),
            pltpu.VMEM(rows, f32),
            pltpu.VMEM(rows, f32),
            pltpu.VMEM(compact, f32),
            pltpu.VMEM((count,) + compact, f32),
            pltpu.VMEM((1, cells), bf16),
            pltpu.VMEM((count, cells // count), bf16),
            dma((2,)),
            dma((2, CHUNKS)),
            dma((2, CHUNKS)),
            dma((count,)),
            dma((count,)),
            dma((count,)),
            dma((count,)),
            dma((count,)),
            dma((count,)),
            dma((2,)),
        ],
        compiler_params=pltpu.CompilerParams(collective_id=1, has_side_effects=True),
        name="exchange_and_projection",
    )(orbitals, trial, occupations, *tables())


def solution(mesh):
    return jax.shard_map(
        local,
        mesh=mesh,
        in_specs=(P(("spin", "band"), None), P(("spin", "band"), None), P(("spin", "band"))),
        out_specs=(P(("spin", "band"), None), P("spin", "band")),
        check_vma=False,
    )
```

```python
import functools
import math

import jax
import jax.numpy as jnp
import numpy as np
from jax import lax
from jax.experimental import pallas as pl
from jax.experimental.pallas import tpu as pltpu
from jax.sharding import PartitionSpec as P

NG = 64
FRACTION = 0.25
OMEGA = 1.0
LANES = 128
TILE = 256
CHUNKS = 4
UNROLL = 2
LAST_UNROLL = 2
VMEM_LIMIT = 30 << 20
WRITTEN_OUT = 32
ORBITAL, SIBLING, TRIAL, RELAY, ONWARD, EXCHANGE, PART = range(7)
KINDS = 7
MESH = pl.DeviceIdType.MESH

HALF = NG // 2
SUB = TILE // HALF
PLANE = NG * NG
ROWS = NG * NG * NG // LANES


def cas_table():
    index = np.arange(NG)
    phases = (index[:, None] * index[None, :] % NG).astype(np.float32) * np.float32(2.0 * math.pi / NG)
    return np.cos(phases) + np.sin(phases)


def tables():
    table = cas_table()
    order = np.concatenate([np.arange(0, NG, 2), np.arange(1, NG, 2)])
    eye = np.eye(TILE // NG, dtype=np.float32)
    sums = np.array([[1.0, 1.0], [1.0, -1.0]], np.float32)
    right_c = np.kron(np.eye(TILE // LANES, dtype=np.float32), np.kron(sums, table))
    left_b = np.kron(eye, table[order][:, order])
    halves = (table[0::2, :HALF], table[1::2, :HALF])
    rows = np.eye(TILE // HALF, dtype=np.float32)
    left_a = np.concatenate([np.kron(half, rows) for half in halves])
    back_a = np.concatenate([np.kron(half.T, rows) for half in halves])
    return jnp.asarray(np.concatenate([left_a, back_a, left_b, right_c])).astype(jnp.bfloat16)


def dot(left, right):
    return jnp.dot(left, right, preferred_element_type=jnp.float32)


def low(value):
    return value.astype(jnp.bfloat16)


def wide(value):
    return value.astype(jnp.float32)


def exchanged(first, second):
    lower = lax.broadcasted_iota(jnp.int32, first.shape, 1) < LANES // 2
    return (
        jnp.where(lower, first, pltpu.roll(second, LANES // 2, 1)),
        jnp.where(lower, pltpu.roll(first, LANES // 2, 1), second),
    )


def wavenum_sq(index):
    modes = wide(jnp.where(2 * index < NG, index, index - NG))
    wavenum = modes * (2.0 * math.pi / NG)
    return wavenum * wavenum


def screened_rows(group):
    shape = (TILE, LANES)
    row = lax.broadcasted_iota(jnp.int32, shape, 0)
    lane = lax.broadcasted_iota(jnp.int32, shape, 1)
    a = 2 * (row // SUB) + lane // NG
    place = group * SUB + row % SUB
    b = 2 * (place % HALF) + place // HALF
    norm_sq = wavenum_sq(a) + wavenum_sq(b) + wavenum_sq(lane % NG)
    bounded = jnp.where(norm_sq > 0, norm_sq, 1.0)
    screened = jnp.where(
        norm_sq > 0,
        4.0 * math.pi / bounded * (1.0 - jnp.exp(-bounded / (4.0 * OMEGA * OMEGA))),
        math.pi / (OMEGA * OMEGA),
    )
    return screened * (1.0 / NG**3)


def partner(me, step, count):
    total, bit = 0, 1
    while bit < count:
        total = total + bit * ((me // bit + step // bit) % 2)
        bit *= 2
    return total


def each(count, number, act):
    if count <= WRITTEN_OUT:
        for i in range(number):
            act(i)
    else:
        pl.loop(0, number)(act)


def grown(total, count):
    shift = LANES // 2
    while shift >= count:
        total = total + pltpu.roll(total, shift, 1)
        shift //= 2
    return total


def own_lanes(count):
    shape = (count, LANES)
    spread = LANES // count
    return (
        lax.broadcasted_iota(jnp.int32, shape, 0) % spread
        == lax.broadcasted_iota(jnp.int32, shape, 1) // count
    )


def own_columns(count):
    return lax.broadcasted_iota(jnp.int32, (count, TILE), 1) // count


def body(
    count,
    orb_hbm, tri_hbm, tables_hbm, occ,
    line_out, low_out, summed,
    factors,
    orb_line, tri_line, own, own_w, sibling, remote, tri_rows, kern, field, acc,
    e_rows, t_in, r_in, e_in, tt, et, exch_line, et_low, part, parts, total_here,
    load_sem, send_sem, recv_sem, orb_recv, e_recv, out_sem,
):
    me = lax.axis_index("band")
    flips = [bit * (1 - 2 * (me // bit % 2)) for bit in (1 << k for k in range(count.bit_length() - 1))]

    def mate(step):
        if isinstance(step, int):
            return me + sum(flip for k, flip in enumerate(flips) if step >> k & 1)
        return partner(me, step, count)

    barrier = pltpu.get_barrier_semaphore()
    slab = ROWS // count
    pack = TILE // count
    spread = LANES // count
    groups = slab // pack
    tiles = ROWS // TILE
    per_tile = TILE // NG
    depth = ROWS // CHUNKS
    span = HALF // CHUNKS * PLANE
    planes = max(count // 4, 1)
    sib = me + 1 - 2 * (me % 2)
    rem = (me + count - 1 + 2 * (me % 2)) % count
    left_a = factors.at[: 2 * TILE]
    back_a = factors.at[2 * TILE : 4 * TILE]
    left_b = factors.at[4 * TILE : 5 * TILE]
    right_c = factors.at[5 * TILE :]
    flat_t = tri_rows.reshape(ROWS, LANES)
    flat_e = e_rows.reshape(ROWS, LANES)

    far = planes - 1

    def far_steps(lows, act):
        def mixed(t):
            upper = t % far
            act((far - upper) * 4 + (t // far + upper) % lows)

        each(count, lows * far, mixed)

    def near_steps(act):
        for step in range(1, min(count, 4)):
            act(step)

    def load_orb(chunk, half):
        at = half * CHUNKS + chunk
        cut = pl.ds(at * span, span)
        return pltpu.make_async_copy(orb_hbm.at[:, cut], orb_line.at[:, cut], load_sem.at[at])

    def plane(ref, a):
        cut = pl.ds(pl.multiple_of(a * PLANE, PLANE), PLANE)
        return wide(ref[:, cut]).reshape(HALF, LANES)

    def remote_copy(src, dst, send, recv, peer):
        return pltpu.make_async_remote_copy(
            src_ref=src,
            dst_ref=dst,
            send_sem=send,
            recv_sem=recv,
            device_id={"band": peer},
            device_id_type=MESH,
        )

    def orbital(chunk):
        cut = pl.ds(chunk * depth, depth)
        return remote_copy(
            own_w.at[cut], remote.at[cut], send_sem.at[ORBITAL], orb_recv.at[chunk], rem
        )

    to_sibling = remote_copy(own_w, sibling, send_sem.at[SIBLING], recv_sem.at[SIBLING], sib)
    orbital_sent = remote_copy(own_w, remote, send_sem.at[ORBITAL], orb_recv.at[0], rem)

    def several(src, dst, kind, number):
        every = pl.ds(0, number)
        return remote_copy(src.at[every], dst.at[every], send_sem.at[kind], recv_sem.at[kind], sib)

    def trial_copy(step):
        peer = mate(step)
        return remote_copy(
            tri_rows.at[peer], t_in.at[me], send_sem.at[TRIAL], recv_sem.at[TRIAL], peer
        )

    def relayed(step):
        peer = mate(step)
        return remote_copy(
            tri_rows.at[mate(step + 2)], r_in.at[me], send_sem.at[RELAY], recv_sem.at[RELAY], peer
        )

    def onward(step):
        source = mate(step)
        return remote_copy(
            r_in.at[source], t_in.at[source], send_sem.at[ONWARD], recv_sem.at[TRIAL], mate(2)
        )

    def exchange_copy(peer, slot):
        return remote_copy(
            e_rows.at[peer], e_in.at[slot], send_sem.at[EXCHANGE], e_recv.at[slot], peer
        )

    def part_copy(peer):
        return remote_copy(part, parts.at[me], send_sem.at[PART], recv_sem.at[PART], peer)

    def tile(group):
        return pl.ds(pl.multiple_of(group * TILE, TILE), TILE)

    def two(read, step):
        return jnp.concatenate([read(2 * step), read(2 * step + 1)], axis=1)

    def halved(value):
        lane = lax.broadcasted_iota(jnp.int32, (TILE, TILE), 1)
        return jnp.where(lane % LANES < LANES // 2, value[:TILE], value[TILE:])

    def rise(weighted, start, stop):
        @pl.loop(start // 2, stop // 2, unroll=min(UNROLL, (stop - start) // 2))
        def _(step):
            density = two(
                lambda group: low(wide(own[tile(group), :]) * wide(weighted[tile(group), :])), step
            )
            value = dot(left_b[...], low(dot(density, right_c[...])))
            field[tile(2 * step), :] = value[:, :LANES]
            field[tile(2 * step + 1), :] = value[:, LANES:]

    def strip(a, group):
        return pl.ds(pl.multiple_of(a * NG + group * SUB, SUB), SUB)

    def turn(unroll):
        @pl.loop(0, tiles // 2, unroll=unroll)
        def _(step):
            value = two(
                lambda group: low(
                    jnp.concatenate([field[strip(a, group), :] for a in range(HALF)], axis=0)
                ),
                step,
            )
            value = low(halved(dot(left_a[...], value)))
            value = low(wide(value) * two(lambda group: kern[tile(group), :], step))
            value = low(halved(dot(back_a[...], value)))
            value = dot(value, right_c[...])
            for side in range(2):
                for a in range(HALF):
                    field[strip(a, 2 * step + side), :] = value[
                        a * SUB : (a + 1) * SUB, side * LANES : (side + 1) * LANES
                    ]

    def fall(weighted, step):
        value = dot(left_b[...], two(lambda group: low(field[tile(group), :]), step))
        return [
            value[:, side * LANES : (side + 1) * LANES] * wide(weighted[tile(2 * step + side), :])
            for side in range(2)
        ]

    load_tables = pltpu.make_async_copy(tables_hbm, factors, load_sem.at[2 * CHUNKS + 1])
    load_tri = pltpu.make_async_copy(tri_hbm, tri_line, load_sem.at[2 * CHUNKS])
    for chunk in range(CHUNKS):
        for half in range(2):
            load_orb(chunk, half).start()

    def greet(i):
        pl.semaphore_signal(
            barrier, inc=1, device_id={"band": mate(i + 1)}, device_id_type=MESH
        )

    each(count, count - 1, greet)

    fill = occ[0:1, :]
    for chunk in range(CHUNKS):
        for half in range(2):
            load_orb(chunk, half).wait()

        @pl.loop(chunk * HALF // CHUNKS, (chunk + 1) * HALF // CHUNKS, unroll=2)
        def _(a):
            pair = jnp.concatenate(exchanged(plane(orb_line, a), plane(orb_line, a + HALF)), axis=0)
            cut = pl.ds(pl.multiple_of(a * NG, NG), NG)
            own[cut, :] = low(pair)
            own_w[cut, :] = low(pair * fill)

    load_tri.start()
    load_tables.start()

    pl.semaphore_wait(barrier, count - 1)
    for chunk in range(CHUNKS):
        orbital(chunk).start()
    to_sibling.start()

    load_tri.wait()

    @pl.loop(0, NG, unroll=2)
    def _(a):
        flat_t[pl.ds(pl.multiple_of(a * HALF, HALF), HALF), :] = low(plane(tri_line, a))

    load_tables.wait()
    trial_copy(1).start()

    def send_trial(step):
        relayed(step).start()
        trial_copy(step).start()

    far_steps(2, send_trial)

    @pl.loop(0, tiles)
    def _(group):
        kern[tile(group), :] = screened_rows(group)

    rise(own_w, 0, tiles)
    turn(UNROLL)

    @pl.loop(0, tiles // 2, unroll=UNROLL)
    def _(step):
        for side, value in enumerate(fall(own_w, step)):
            acc[tile(2 * step + side), :] = value

    to_sibling.wait_recv()
    rise(sibling, 0, tiles)
    turn(UNROLL)

    @pl.loop(0, tiles // 2, unroll=UNROLL)
    def _(step):
        for side, value in enumerate(fall(sibling, step)):
            acc[tile(2 * step + side), :] += value

    for chunk in range(CHUNKS - 1):
        orbital(chunk).wait_recv()
        rise(remote, chunk * tiles // CHUNKS, (chunk + 1) * tiles // CHUNKS)
    orbital(CHUNKS - 1).wait_recv()
    for step in range(2, min(count, 4)):
        trial_copy(step).start()
    rise(remote, tiles - tiles // CHUNKS, tiles)
    turn(LAST_UNROLL)

    @pl.loop(0, tiles // 2, unroll=UNROLL)
    def _(step):
        for side, value in enumerate(fall(remote, step)):
            group = 2 * step + side
            value = -FRACTION * (acc[tile(group), :] + value)
            for j in range(per_tile):
                a = group * per_tile + j
                first, second = exchanged(
                    value[j * NG : j * NG + HALF], value[j * NG + HALF : (j + 1) * NG]
                )
                flat_e[pl.ds(pl.multiple_of(a * HALF, HALF), HALF), :] = low(first)
                flat_e[pl.ds(pl.multiple_of((a + HALF) * HALF, HALF), HALF), :] = low(second)

    t_in[pl.ds(me, 1)] = tri_rows[pl.ds(me, 1)]
    e_in[pl.ds(me, 1)] = e_rows[pl.ds(me, 1)]
    def send_exchange(step):
        exchange_copy(mate(step), me).start()

    near_steps(send_exchange)
    far_steps(4, send_exchange)

    def spread_out(src, dst, slot):
        dst[pl.ds(slot, slab, stride=count), :] = wide(src[slot])

    def take_exchange(step):
        peer = mate(step)
        exchange_copy(peer, peer).wait_recv()
        spread_out(e_in, et, peer)

    if far > 0:
        several(r_in, r_in, RELAY, 2 * far).wait_recv()
        far_steps(2, lambda step: onward(step).start())

    @pl.loop(0, NG, unroll=2)
    def _(a):
        cut = pl.ds(pl.multiple_of(a * PLANE, PLANE), PLANE)
        rows = wide(flat_e[pl.ds(pl.multiple_of(a * HALF, HALF), HALF), :])
        exch_line[:, cut] = low(rows.reshape(1, PLANE))

    store_line = pltpu.make_async_copy(exch_line, line_out, out_sem.at[0])
    store_low = pltpu.make_async_copy(et_low, low_out, out_sem.at[1])
    store_line.start()
    several(tri_rows, t_in, TRIAL, count - 1).wait_recv()

    @pl.loop(0, count)
    def _(slot):
        spread_out(t_in, tt, slot)

    spread_out(e_in, et, me)
    near_steps(take_exchange)
    far_steps(4, take_exchange)

    mine = [low(et[g * TILE : (g + 1) * TILE, :]) for g in range(groups)]
    for g in range(groups):
        et_low[g * TILE : (g + 1) * TILE, :] = mine[g]
    gram = lax.dot_general(
        jnp.concatenate([low(tt[g * TILE : (g + 1) * TILE, :]) for g in range(groups)], axis=1),
        jnp.concatenate(mine, axis=1),
        (((1,), (1,)), ((), ())),
        preferred_element_type=jnp.float32,
    )
    column = own_columns(count)
    total = jnp.zeros((count, TILE), jnp.float32)
    for r in range(pack):
        total = total + jnp.where(column == r, gram[r * count : (r + 1) * count], 0.0)
    total = grown(total[:, :LANES] + total[:, LANES:], count)
    if spread > 1:
        total = jnp.sum(
            jnp.where(own_lanes(count), total, 0.0).reshape(count // spread, spread, LANES), axis=1
        )
    part[...] = total
    parts[pl.ds(me, 1)] = total[None]

    each(count, count - 1, lambda i: part_copy(mate(count - 1 - i)).start())
    store_low.start()
    orbital_sent.wait_send()
    to_sibling.wait_send()
    several(tri_rows, t_in, TRIAL, count - 1 - 2 * far).wait_send()
    if far > 0:
        several(tri_rows, r_in, RELAY, 2 * far).wait_send()
        several(r_in, t_in, ONWARD, 2 * far).wait_send()
    several(e_rows, e_in, EXCHANGE, count - 1).wait_send()
    store_line.wait()
    store_low.wait()
    several(parts, parts, PART, count - 1).wait()
    total_here[...] = jnp.sum(parts[...], axis=0)
    store_sum = pltpu.make_async_copy(total_here, summed, out_sem.at[2])
    store_sum.start()
    store_sum.wait()


def finish(count, exch_line, et_low, summed, exch_hbm, proj_hbm, proj, out_sem):
    pack = TILE // count
    spread = LANES // count
    groups = ROWS // TILE
    width = pack * LANES
    store_exch = pltpu.make_async_copy(exch_line, exch_hbm, out_sem.at[groups])
    store_exch.start()
    total = summed[...] / math.sqrt(ROWS * LANES)
    if spread > 1:
        total = jnp.broadcast_to(total[:, None, :], (count // spread, spread, LANES))
        total = jnp.where(own_lanes(count), total.reshape(count, LANES), 0.0)
    total = grown(total, count)
    total = jnp.concatenate([total, total], axis=1)
    column = own_columns(count)
    mixing = low(
        jnp.concatenate([jnp.where(column == r, total, 0.0) for r in range(pack)], axis=0)
    )
    stores = []
    for group in range(groups):
        piece = dot(mixing, et_low[group * TILE : (group + 1) * TILE, :])
        piece = low(piece * (-1.0 / math.sqrt(count)))
        for r in range(pack):
            at = (group * pack + r) * LANES
            proj[:, at : at + LANES] = piece[r * count : (r + 1) * count]
        cut = pl.ds(group * width, width)
        stores.append(
            pltpu.make_async_copy(proj.at[:, cut], proj_hbm.at[:, cut], out_sem.at[group])
        )
        stores[-1].start()
    for store in stores:
        store.wait()
    store_exch.wait()


def local(orbitals, trial, occupations):
    count = lax.axis_size("band")
    cells = orbitals.shape[1]
    slab = ROWS // count
    rows = (ROWS, LANES)
    bf16, f32 = jnp.bfloat16, jnp.float32
    compact = (count // (LANES // count), LANES)
    dma = pltpu.SemaphoreType.DMA
    anywhere = pl.BlockSpec(memory_space=pl.ANY)
    vmem = pl.BlockSpec(memory_space=pltpu.VMEM)
    consts = tables()
    line, spread_low, summed = pl.pallas_call(
        functools.partial(body, count),
        out_shape=(
            jax.ShapeDtypeStruct((1, cells), bf16),
            jax.ShapeDtypeStruct(rows, bf16),
            jax.ShapeDtypeStruct(compact, f32),
        ),
        in_specs=[pl.BlockSpec(memory_space=pltpu.HBM)] * 3 + [vmem],
        out_specs=(anywhere, anywhere, anywhere),
        scratch_shapes=[
            pltpu.VMEM(consts.shape, bf16),
            pltpu.VMEM((1, cells), bf16),
            pltpu.VMEM((1, cells), bf16),
            pltpu.VMEM(rows, bf16),
            pltpu.VMEM(rows, bf16),
            pltpu.VMEM(rows, bf16),
            pltpu.VMEM(rows, bf16),
            pltpu.VMEM((count, slab, LANES), bf16),
            pltpu.VMEM(rows, f32),
            pltpu.VMEM(rows, f32),
            pltpu.VMEM(rows, f32),
            pltpu.VMEM((count, slab, LANES), bf16),
            pltpu.VMEM((count, slab, LANES), bf16),
            pltpu.VMEM((count, slab, LANES), bf16),
            pltpu.VMEM((count, slab, LANES), bf16),
            pltpu.VMEM(rows, f32),
            pltpu.VMEM(rows, f32),
            pltpu.VMEM((1, cells), bf16),
            pltpu.VMEM(rows, bf16),
            pltpu.VMEM(compact, f32),
            pltpu.VMEM((count,) + compact, f32),
            pltpu.VMEM(compact, f32),
            dma((2 * CHUNKS + 2,)),
            dma((KINDS,)),
            dma((KINDS,)),
            dma((CHUNKS,)),
            dma((count,)),
            dma((3,)),
        ],
        compiler_params=pltpu.CompilerParams(
            collective_id=1, has_side_effects=True, vmem_limit_bytes=VMEM_LIMIT
        ),
        name="exchange",
    )(
        *[pltpu.with_memory_space_constraint(x, pltpu.HBM) for x in (orbitals, trial, consts)],
        jnp.broadcast_to(occupations.astype(f32)[:, None], (8, LANES)),
    )
    return pl.pallas_call(
        functools.partial(finish, count),
        out_shape=(
            jax.ShapeDtypeStruct((1, cells), bf16),
            jax.ShapeDtypeStruct((count, cells // count), bf16),
        ),
        in_specs=[vmem, vmem, vmem],
        out_specs=(anywhere, anywhere),
        scratch_shapes=[
            pltpu.VMEM((count, cells // count), bf16),
            dma((ROWS // TILE + 1,)),
        ],
        compiler_params=pltpu.CompilerParams(vmem_limit_bytes=VMEM_LIMIT),
        name="finish",
    )(line, spread_low, summed)


def solution(mesh):
    return jax.shard_map(
        local,
        mesh=mesh,
        in_specs=(P(("spin", "band"), None), P(("spin", "band"), None), P(("spin", "band"))),
        out_specs=(P(("spin", "band"), None), P("spin", "band")),
        check_vma=False,
    )
```

```python
import functools
import math

import jax
import jax.numpy as jnp
import numpy as np
from jax import lax
from jax.experimental import pallas as pl
from jax.experimental.pallas import tpu as pltpu
from jax.sharding import PartitionSpec as P

NG = 64
FRACTION = 0.25
OMEGA = 1.0
LANES = 128
TILE = 256
CHUNKS = 4
UNROLL = 2
LAST_UNROLL = 2
VMEM_LIMIT = 30 << 20
WRITTEN_OUT = 32
PIECES = 1
LOADS = 2
OWN, TRIAL, PART, ONWARD, EXCHANGE = range(5)
MESH = pl.DeviceIdType.MESH

HALF = NG // 2
SUB = TILE // HALF
PLANE = NG * NG
ROWS = NG * NG * NG // LANES


def cas_table():
    index = np.arange(NG)
    phases = (index[:, None] * index[None, :] % NG).astype(np.float32) * np.float32(2.0 * math.pi / NG)
    return np.cos(phases) + np.sin(phases)


def tables():
    table = cas_table()
    order = np.concatenate([np.arange(0, NG, 2), np.arange(1, NG, 2)])
    eye = np.eye(TILE // NG, dtype=np.float32)
    sums = np.array([[1.0, 1.0], [1.0, -1.0]], np.float32)
    right_c = np.kron(np.eye(TILE // LANES, dtype=np.float32), np.kron(sums, table))
    left_b = np.kron(eye, table[order][:, order])
    halves = (table[0::2, :HALF], table[1::2, :HALF])
    rows = np.eye(TILE // HALF, dtype=np.float32)
    left_a = np.concatenate([np.kron(half, rows) for half in halves])
    back_a = np.concatenate([np.kron(half.T, rows) for half in halves])
    return jnp.asarray(np.concatenate([left_a, back_a, left_b, right_c])).astype(jnp.bfloat16)


def dot(left, right):
    return jnp.dot(left, right, preferred_element_type=jnp.float32)


def low(value):
    return value.astype(jnp.bfloat16)


def wide(value):
    return value.astype(jnp.float32)


def exchanged(first, second):
    lower = lax.broadcasted_iota(jnp.int32, first.shape, 1) < LANES // 2
    return (
        jnp.where(lower, first, pltpu.roll(second, LANES // 2, 1)),
        jnp.where(lower, pltpu.roll(first, LANES // 2, 1), second),
    )


def wavenum_sq(index):
    modes = wide(jnp.where(2 * index < NG, index, index - NG))
    wavenum = modes * (2.0 * math.pi / NG)
    return wavenum * wavenum


def screened_rows(group):
    shape = (TILE, LANES)
    row = lax.broadcasted_iota(jnp.int32, shape, 0)
    lane = lax.broadcasted_iota(jnp.int32, shape, 1)
    a = 2 * (row // SUB) + lane // NG
    place = group * SUB + row % SUB
    b = 2 * (place % HALF) + place // HALF
    norm_sq = wavenum_sq(a) + wavenum_sq(b) + wavenum_sq(lane % NG)
    bounded = jnp.where(norm_sq > 0, norm_sq, 1.0)
    screened = jnp.where(
        norm_sq > 0,
        4.0 * math.pi / bounded * (1.0 - jnp.exp(-bounded / (4.0 * OMEGA * OMEGA))),
        math.pi / (OMEGA * OMEGA),
    )
    return screened * (1.0 / NG**3)


def partner(me, step, count):
    total, bit = 0, 1
    while bit < count:
        total = total + bit * ((me // bit + step // bit) % 2)
        bit *= 2
    return total


def each(count, number, act):
    if count <= WRITTEN_OUT:
        for i in range(number):
            act(i)
    else:
        pl.loop(0, number)(act)


def grown(total, count):
    shift = LANES // 2
    while shift >= count:
        total = total + pltpu.roll(total, shift, 1)
        shift //= 2
    return total


def own_lanes(count):
    shape = (count, LANES)
    spread = LANES // count
    return (
        lax.broadcasted_iota(jnp.int32, shape, 0) % spread
        == lax.broadcasted_iota(jnp.int32, shape, 1) // count
    )


def own_columns(count):
    return lax.broadcasted_iota(jnp.int32, (count, TILE), 1) // count


def body(
    count,
    orb_hbm, tri_hbm, tables_hbm, occ,
    line_out, low_out, summed,
    factors,
    orb_line, tri_line, own, own_w, sibling, remote, tri_rows, kern, field, acc,
    e_rows, t_in, r_in, e_in, tt, et, exch_line, et_low, part, parts, total_here,
    load_sem, send_sem, recv_sem, orb_recv, r_recv, e_recv, out_sem,
):
    me = lax.axis_index("band")
    flips = [bit * (1 - 2 * (me // bit % 2)) for bit in (1 << k for k in range(count.bit_length() - 1))]

    def mate(step):
        if isinstance(step, int):
            return me + sum(flip for k, flip in enumerate(flips) if step >> k & 1)
        return partner(me, step, count)

    barrier = pltpu.get_barrier_semaphore()
    slab = ROWS // count
    pack = TILE // count
    spread = LANES // count
    groups = slab // pack
    tiles = ROWS // TILE
    per_tile = TILE // NG
    depth = ROWS // CHUNKS
    span = HALF // LOADS * PLANE
    planes = max(count // 4, 1)
    sib = me + 1 - 2 * (me % 2)
    rem = (me + count - 1 + 2 * (me % 2)) % count
    left_a = factors.at[: 2 * TILE]
    back_a = factors.at[2 * TILE : 4 * TILE]
    left_b = factors.at[4 * TILE : 5 * TILE]
    right_c = factors.at[5 * TILE :]
    flat_t = tri_rows.reshape(ROWS, LANES)
    flat_e = e_rows.reshape(ROWS, LANES)

    far = planes - 1

    def far_steps(lows, act):
        def mixed(t):
            upper = t % far
            act((far - upper) * 4 + (t // far + upper) % lows)

        each(count, lows * far, mixed)

    def far_first(lows, act):
        each(count, lows * far, lambda t: act((far - t // lows) * 4 + t % lows))

    def near_steps(act):
        for step in range(1, min(count, 4)):
            act(step)

    def load_orb(piece, half):
        cut = pl.ds((half * LOADS + piece) * span, span)
        return pltpu.make_async_copy(orb_hbm.at[:, cut], orb_line.at[:, cut], load_sem.at[piece])

    def loaded_orb(piece):
        cut = pl.ds(0, 2 * span)
        return pltpu.make_async_copy(orb_hbm.at[:, cut], orb_line.at[:, cut], load_sem.at[piece])

    def plane(ref, a):
        cut = pl.ds(pl.multiple_of(a * PLANE, PLANE), PLANE)
        return wide(ref[:, cut]).reshape(HALF, LANES)

    def remote_copy(src, dst, send, recv, peer):
        return pltpu.make_async_remote_copy(
            src_ref=src,
            dst_ref=dst,
            send_sem=send,
            recv_sem=recv,
            device_id={"band": peer},
            device_id_type=MESH,
        )

    def orbital(chunk):
        cut = pl.ds(chunk * depth, depth)
        return remote_copy(
            own_w.at[cut], remote.at[cut], send_sem.at[OWN], orb_recv.at[chunk], rem
        )

    to_sibling = remote_copy(own_w, sibling, send_sem.at[OWN], recv_sem.at[OWN], sib)
    own_sent = remote_copy(kern, field, send_sem.at[OWN], recv_sem.at[OWN], sib)

    def several(src, dst, kind, number):
        every = pl.ds(0, number)
        return remote_copy(
            src.at[every], dst.at[every], send_sem.at[kind], recv_sem.at[min(kind, PART)], sib
        )

    def trial_copy(step):
        peer = mate(step)
        return remote_copy(
            tri_rows.at[peer], t_in.at[me], send_sem.at[TRIAL], recv_sem.at[TRIAL], peer
        )

    def relay_copy(step, slot):
        return remote_copy(
            tri_rows.at[mate(step + 2)],
            r_in.at[slot],
            send_sem.at[TRIAL],
            r_recv.at[(step // 4 - 1) * 2 + step % 2],
            mate(step),
        )

    def onward(step):
        source = mate(step)
        return remote_copy(
            r_in.at[source], t_in.at[source], send_sem.at[ONWARD], recv_sem.at[TRIAL], mate(2)
        )

    def exchange_copy(step, slot):
        peer = mate(step)
        return remote_copy(
            e_rows.at[peer], e_in.at[slot], send_sem.at[EXCHANGE], e_recv.at[step - 1], peer
        )

    def part_copy(peer):
        return remote_copy(part, parts.at[me], send_sem.at[PART], recv_sem.at[PART], peer)

    def tile(group):
        return pl.ds(pl.multiple_of(group * TILE, TILE), TILE)

    def two(read, step):
        return jnp.concatenate([read(2 * step), read(2 * step + 1)], axis=1)

    def halved(value):
        lane = lax.broadcasted_iota(jnp.int32, (TILE, TILE), 1)
        return jnp.where(lane % LANES < LANES // 2, value[:TILE], value[TILE:])

    def rise(weighted, start, stop):
        @pl.loop(start // 2, stop // 2, unroll=min(UNROLL, (stop - start) // 2))
        def _(step):
            density = two(
                lambda group: low(wide(own[tile(group), :]) * wide(weighted[tile(group), :])), step
            )
            value = dot(left_b[...], low(dot(density, right_c[...])))
            field[tile(2 * step), :] = value[:, :LANES]
            field[tile(2 * step + 1), :] = value[:, LANES:]

    def strip(a, group):
        return pl.ds(pl.multiple_of(a * NG + group * SUB, SUB), SUB)

    def turn(unroll):
        @pl.loop(0, tiles // 2, unroll=unroll)
        def _(step):
            value = two(
                lambda group: low(
                    jnp.concatenate([field[strip(a, group), :] for a in range(HALF)], axis=0)
                ),
                step,
            )
            value = low(halved(dot(left_a[...], value)))
            value = low(wide(value) * two(lambda group: kern[tile(group), :], step))
            value = low(halved(dot(back_a[...], value)))
            value = dot(value, right_c[...])
            for side in range(2):
                for a in range(HALF):
                    field[strip(a, 2 * step + side), :] = value[
                        a * SUB : (a + 1) * SUB, side * LANES : (side + 1) * LANES
                    ]

    def fall(weighted, step):
        value = dot(left_b[...], two(lambda group: low(field[tile(group), :]), step))
        return [
            value[:, side * LANES : (side + 1) * LANES] * wide(weighted[tile(2 * step + side), :])
            for side in range(2)
        ]

    load_tables = pltpu.make_async_copy(tables_hbm, factors, load_sem.at[LOADS + 1])
    load_tri = pltpu.make_async_copy(tri_hbm, tri_line, load_sem.at[LOADS])

    def greet(i):
        pl.semaphore_signal(
            barrier, inc=1, device_id={"band": mate(i + 1)}, device_id_type=MESH
        )

    each(count, count - 1, lambda i: greet(count - 2 - i))

    for piece in range(LOADS):
        for half in range(2):
            load_orb(piece, half).start()
    load_tri.start()
    load_tables.start()

    fill = occ[0:1, :]
    for piece in range(LOADS):
        loaded_orb(piece).wait()

        @pl.loop(piece * HALF // LOADS, (piece + 1) * HALF // LOADS, unroll=2)
        def _(a):
            pair = jnp.concatenate(exchanged(plane(orb_line, a), plane(orb_line, a + HALF)), axis=0)
            cut = pl.ds(pl.multiple_of(a * NG, NG), NG)
            own[cut, :] = low(pair)
            own_w[cut, :] = low(pair * fill)


    load_tri.wait()

    @pl.loop(0, NG, unroll=2)
    def _(a):
        flat_t[pl.ds(pl.multiple_of(a * HALF, HALF), HALF), :] = low(plane(tri_line, a))

    load_tables.wait()
    pl.semaphore_wait(barrier, count - 1)
    for chunk in range(CHUNKS):
        orbital(chunk).start()
    to_sibling.start()

    trial_copy(1).start()

    def send_trial(step):
        relay_copy(step, me).start()
        trial_copy(step).start()

    far_first(2, send_trial)

    @pl.loop(0, tiles)
    def _(group):
        kern[tile(group), :] = screened_rows(group)

    rise(own_w, 0, tiles)
    turn(UNROLL)

    @pl.loop(0, tiles // 2, unroll=UNROLL)
    def _(step):
        for side, value in enumerate(fall(own_w, step)):
            acc[tile(2 * step + side), :] = value

    to_sibling.wait_recv()
    rise(sibling, 0, tiles)
    turn(UNROLL)

    @pl.loop(0, tiles // 2, unroll=UNROLL)
    def _(step):
        for side, value in enumerate(fall(sibling, step)):
            acc[tile(2 * step + side), :] += value

    for chunk in range(CHUNKS - 1):
        orbital(chunk).wait_recv()
        rise(remote, chunk * tiles // CHUNKS, (chunk + 1) * tiles // CHUNKS)
    orbital(CHUNKS - 1).wait_recv()
    for step in range(2, min(count, 4)):
        trial_copy(step).start()
    rise(remote, tiles - tiles // CHUNKS, tiles)
    turn(LAST_UNROLL)

    @pl.loop(0, tiles // 2, unroll=UNROLL)
    def _(step):
        for side, value in enumerate(fall(remote, step)):
            group = 2 * step + side
            value = -FRACTION * (acc[tile(group), :] + value)
            for j in range(per_tile):
                a = group * per_tile + j
                first, second = exchanged(
                    value[j * NG : j * NG + HALF], value[j * NG + HALF : (j + 1) * NG]
                )
                flat_e[pl.ds(pl.multiple_of(a * HALF, HALF), HALF), :] = low(first)
                flat_e[pl.ds(pl.multiple_of((a + HALF) * HALF, HALF), HALF), :] = low(second)

    t_in[pl.ds(me, 1)] = tri_rows[pl.ds(me, 1)]
    e_in[pl.ds(me, 1)] = e_rows[pl.ds(me, 1)]
    def send_exchange(step):
        exchange_copy(step, me).start()

    near_steps(send_exchange)
    far_steps(4, send_exchange)

    def spread_out(src, dst, slot):
        dst[pl.ds(slot, slab, stride=count), :] = wide(src[slot])

    def take_exchange(step):
        peer = mate(step)
        exchange_copy(step, peer).wait_recv()
        spread_out(e_in, et, peer)

    @pl.loop(0, NG, unroll=2)
    def _(a):
        cut = pl.ds(pl.multiple_of(a * PLANE, PLANE), PLANE)
        rows = wide(flat_e[pl.ds(pl.multiple_of(a * HALF, HALF), HALF), :])
        exch_line[:, cut] = low(rows.reshape(1, PLANE))

    store_line = pltpu.make_async_copy(exch_line, line_out, out_sem.at[0])
    store_low = pltpu.make_async_copy(et_low, low_out, out_sem.at[1])
    store_line.start()
    def pass_on(step):
        relay_copy(step, mate(step)).wait_recv()
        onward(step).start()

    far_first(2, pass_on)
    several(tri_rows, t_in, TRIAL, count - 1).wait_recv()

    @pl.loop(0, count, unroll=4)
    def _(slot):
        spread_out(t_in, et, slot)

    @pl.loop(0, tiles, unroll=4)
    def _(group):
        tt[tile(group), :] = low(et[tile(group), :])

    spread_out(e_in, et, me)
    near_steps(take_exchange)
    far_steps(4, take_exchange)

    mine = [low(et[g * TILE : (g + 1) * TILE, :]) for g in range(groups)]
    for g in range(groups):
        et_low[g * TILE : (g + 1) * TILE, :] = mine[g]
    gram = lax.dot_general(
        jnp.concatenate([tt[g * TILE : (g + 1) * TILE, :] for g in range(groups)], axis=1),
        jnp.concatenate(mine, axis=1),
        (((1,), (1,)), ((), ())),
        preferred_element_type=jnp.float32,
    )
    column = own_columns(count)
    total = jnp.zeros((count, TILE), jnp.float32)
    for r in range(pack):
        total = total + jnp.where(column == r, gram[r * count : (r + 1) * count], 0.0)
    total = grown(total[:, :LANES] + total[:, LANES:], count)
    if spread > 1:
        total = jnp.sum(
            jnp.where(own_lanes(count), total, 0.0).reshape(count // spread, spread, LANES), axis=1
        )
    part[...] = total
    parts[pl.ds(me, 1)] = total[None]

    each(count, count - 1, lambda i: part_copy(mate(count - 1 - i)).start())
    store_low.start()
    own_sent.wait_send()
    several(tri_rows, t_in, TRIAL, count - 1).wait_send()
    if far > 0:
        several(r_in, t_in, ONWARD, 2 * far).wait_send()
    several(e_rows, e_in, EXCHANGE, count - 1).wait_send()
    store_line.wait()
    store_low.wait()
    several(parts, parts, PART, count - 1).wait()
    total_here[...] = jnp.sum(parts[...], axis=0)
    store_sum = pltpu.make_async_copy(total_here, summed, out_sem.at[2])
    store_sum.start()
    store_sum.wait()


def finish(count, exch_line, et_low, summed, exch_hbm, proj_hbm, proj, out_sem):
    pack = TILE // count
    spread = LANES // count
    groups = ROWS // TILE
    width = pack * LANES
    stores = []
    part = exch_line.shape[1] // PIECES
    for piece in range(PIECES):
        cut = pl.ds(piece * part, part)
        stores.append(
            pltpu.make_async_copy(
                exch_line.at[:, cut], exch_hbm.at[:, cut], out_sem.at[groups + piece]
            )
        )
        stores[-1].start()
    total = summed[...] / math.sqrt(ROWS * LANES)
    if spread > 1:
        total = jnp.broadcast_to(total[:, None, :], (count // spread, spread, LANES))
        total = jnp.where(own_lanes(count), total.reshape(count, LANES), 0.0)
    total = grown(total, count)
    total = jnp.concatenate([total, total], axis=1)
    column = own_columns(count)
    mixing = low(
        jnp.concatenate([jnp.where(column == r, total, 0.0) for r in range(pack)], axis=0)
    )
    for group in range(groups):
        piece = dot(mixing, et_low[group * TILE : (group + 1) * TILE, :])
        piece = low(piece * (-1.0 / math.sqrt(count)))
        for r in range(pack):
            at = (group * pack + r) * LANES
            proj[:, at : at + LANES] = piece[r * count : (r + 1) * count]
        cut = pl.ds(group * width, width)
        stores.append(
            pltpu.make_async_copy(proj.at[:, cut], proj_hbm.at[:, cut], out_sem.at[group])
        )
        stores[-1].start()
    for store in stores:
        store.wait()


def local(orbitals, trial, occupations):
    count = lax.axis_size("band")
    cells = orbitals.shape[1]
    slab = ROWS // count
    rows = (ROWS, LANES)
    bf16, f32 = jnp.bfloat16, jnp.float32
    compact = (count // (LANES // count), LANES)
    dma = pltpu.SemaphoreType.DMA
    anywhere = pl.BlockSpec(memory_space=pl.ANY)
    vmem = pl.BlockSpec(memory_space=pltpu.VMEM)
    consts = tables()
    line, spread_low, summed = pl.pallas_call(
        functools.partial(body, count),
        out_shape=(
            jax.ShapeDtypeStruct((1, cells), bf16),
            jax.ShapeDtypeStruct(rows, bf16),
            jax.ShapeDtypeStruct(compact, f32),
        ),
        in_specs=[pl.BlockSpec(memory_space=pltpu.HBM)] * 3 + [vmem],
        out_specs=(anywhere, anywhere, anywhere),
        scratch_shapes=[
            pltpu.VMEM(consts.shape, bf16),
            pltpu.VMEM((1, cells), bf16),
            pltpu.VMEM((1, cells), bf16),
            pltpu.VMEM(rows, bf16),
            pltpu.VMEM(rows, bf16),
            pltpu.VMEM(rows, bf16),
            pltpu.VMEM(rows, bf16),
            pltpu.VMEM((count, slab, LANES), bf16),
            pltpu.VMEM(rows, f32),
            pltpu.VMEM(rows, f32),
            pltpu.VMEM(rows, f32),
            pltpu.VMEM((count, slab, LANES), bf16),
            pltpu.VMEM((count, slab, LANES), bf16),
            pltpu.VMEM((count, slab, LANES), bf16),
            pltpu.VMEM((count, slab, LANES), bf16),
            pltpu.VMEM(rows, bf16),
            pltpu.VMEM(rows, f32),
            pltpu.VMEM((1, cells), bf16),
            pltpu.VMEM(rows, bf16),
            pltpu.VMEM(compact, f32),
            pltpu.VMEM((count,) + compact, f32),
            pltpu.VMEM(compact, f32),
            dma((LOADS + 2,)),
            dma((5,)),
            dma((3,)),
            dma((CHUNKS,)),
            dma((max(2 * (count // 4 - 1), 1),)),
            dma((count - 1,)),
            dma((3,)),
        ],
        compiler_params=pltpu.CompilerParams(
            collective_id=1, has_side_effects=True, vmem_limit_bytes=VMEM_LIMIT
        ),
        name="exchange",
    )(
        *[pltpu.with_memory_space_constraint(x, pltpu.HBM) for x in (orbitals, trial, consts)],
        jnp.broadcast_to(occupations.astype(f32)[:, None], (8, LANES)),
    )
    return pl.pallas_call(
        functools.partial(finish, count),
        out_shape=(
            jax.ShapeDtypeStruct((1, cells), bf16),
            jax.ShapeDtypeStruct((count, cells // count), bf16),
        ),
        in_specs=[vmem, vmem, vmem],
        out_specs=(anywhere, anywhere),
        scratch_shapes=[
            pltpu.VMEM((count, cells // count), bf16),
            dma((ROWS // TILE + PIECES,)),
        ],
        compiler_params=pltpu.CompilerParams(vmem_limit_bytes=VMEM_LIMIT),
        name="finish",
    )(line, spread_low, summed)


def solution(mesh):
    return jax.shard_map(
        local,
        mesh=mesh,
        in_specs=(P(("spin", "band"), None), P(("spin", "band"), None), P(("spin", "band"))),
        out_specs=(P(("spin", "band"), None), P("spin", "band")),
        check_vma=False,
    )
```

```python
import functools
import math

import jax
import jax.numpy as jnp
import numpy as np
from jax import lax
from jax.experimental import pallas as pl
from jax.experimental.pallas import tpu as pltpu
from jax.sharding import PartitionSpec as P

NG = 64
FRACTION = 0.25
OMEGA = 1.0
LANES = 128
TILE = 256
CHUNKS = 4
UNROLL = 2
LAST_UNROLL = 2
VMEM_LIMIT = 30 << 20
WRITTEN_OUT = 32
PIECES = 1
LOADS = 2
OWN, TRIAL, PART, ONWARD, EXCHANGE = range(5)
MESH = pl.DeviceIdType.MESH

HALF = NG // 2
SUB = TILE // HALF
PLANE = NG * NG
ROWS = NG * NG * NG // LANES


def cas_table():
    index = np.arange(NG)
    phases = (index[:, None] * index[None, :] % NG).astype(np.float32) * np.float32(2.0 * math.pi / NG)
    return np.cos(phases) + np.sin(phases)


def tables():
    table = cas_table()
    order = np.concatenate([np.arange(0, NG, 2), np.arange(1, NG, 2)])
    eye = np.eye(TILE // NG, dtype=np.float32)
    sums = np.array([[1.0, 1.0], [1.0, -1.0]], np.float32)
    right_c = np.kron(np.eye(TILE // LANES, dtype=np.float32), np.kron(sums, table))
    left_b = np.kron(eye, table[order][:, order])
    halves = (table[0::2, :HALF], table[1::2, :HALF])
    rows = np.eye(TILE // HALF, dtype=np.float32)
    left_a = np.concatenate([np.kron(half, rows) for half in halves])
    back_a = np.concatenate([np.kron(half.T, rows) for half in halves])
    return jnp.asarray(np.concatenate([left_a, back_a, left_b, right_c])).astype(jnp.bfloat16)


def dot(left, right):
    return jnp.dot(left, right, preferred_element_type=jnp.float32)


def low(value):
    return value.astype(jnp.bfloat16)


def wide(value):
    return value.astype(jnp.float32)


def exchanged(first, second):
    lower = lax.broadcasted_iota(jnp.int32, first.shape, 1) < LANES // 2
    return (
        jnp.where(lower, first, pltpu.roll(second, LANES // 2, 1)),
        jnp.where(lower, pltpu.roll(first, LANES // 2, 1), second),
    )


def wavenum_sq(index):
    modes = wide(jnp.where(2 * index < NG, index, index - NG))
    wavenum = modes * (2.0 * math.pi / NG)
    return wavenum * wavenum


def screened_rows(group):
    shape = (TILE, LANES)
    row = lax.broadcasted_iota(jnp.int32, shape, 0)
    lane = lax.broadcasted_iota(jnp.int32, shape, 1)
    a = 2 * (row // SUB) + lane // NG
    place = group * SUB + row % SUB
    b = 2 * (place % HALF) + place // HALF
    norm_sq = wavenum_sq(a) + wavenum_sq(b) + wavenum_sq(lane % NG)
    bounded = jnp.where(norm_sq > 0, norm_sq, 1.0)
    screened = jnp.where(
        norm_sq > 0,
        4.0 * math.pi / bounded * (1.0 - jnp.exp(-bounded / (4.0 * OMEGA * OMEGA))),
        math.pi / (OMEGA * OMEGA),
    )
    return screened * (1.0 / NG**3)


def partner(me, step, count):
    total, bit = 0, 1
    while bit < count:
        total = total + bit * ((me // bit + step // bit) % 2)
        bit *= 2
    return total


def each(count, number, act):
    if count <= WRITTEN_OUT:
        for i in range(number):
            act(i)
    else:
        pl.loop(0, number)(act)


def grown(total, count):
    shift = LANES // 2
    while shift >= count:
        total = total + pltpu.roll(total, shift, 1)
        shift //= 2
    return total


def own_lanes(count):
    shape = (count, LANES)
    spread = LANES // count
    return (
        lax.broadcasted_iota(jnp.int32, shape, 0) % spread
        == lax.broadcasted_iota(jnp.int32, shape, 1) // count
    )


def body(
    count,
    orb_hbm, tri_hbm, tables_hbm, occ,
    line_out, low_out, summed,
    factors,
    orb_line, tri_line, own, own_w, sibling, remote, tri_rows, kern, field, acc,
    e_rows, t_in, r_in, e_in, tt, et, exch_line, et_low, part, parts, total_here,
    load_sem, send_sem, recv_sem, orb_recv, r_recv, e_recv, out_sem,
):
    me = lax.axis_index("band")
    flips = [bit * (1 - 2 * (me // bit % 2)) for bit in (1 << k for k in range(count.bit_length() - 1))]

    def mate(step):
        if isinstance(step, int):
            return me + sum(flip for k, flip in enumerate(flips) if step >> k & 1)
        return partner(me, step, count)

    barrier = pltpu.get_barrier_semaphore()
    slab = ROWS // count
    spread = LANES // count
    tiles = ROWS // TILE
    per_tile = TILE // NG
    depth = ROWS // CHUNKS
    span = HALF // LOADS * PLANE
    planes = max(count // 4, 1)
    sib = me + 1 - 2 * (me % 2)
    rem = (me + count - 1 + 2 * (me % 2)) % count
    left_a = factors.at[: 2 * TILE]
    back_a = factors.at[2 * TILE : 4 * TILE]
    left_b = factors.at[4 * TILE : 5 * TILE]
    right_c = factors.at[5 * TILE :]
    flat_t = tri_rows.reshape(ROWS, LANES)
    flat_e = e_rows.reshape(ROWS, LANES)

    far = planes - 1

    def far_steps(lows, act):
        def mixed(t):
            upper = t % far
            act((1 + upper) * 4 + (t // far + 2 * upper) % lows)

        each(count, lows * far, mixed)

    def far_first(lows, act):
        each(count, lows * far, lambda t: act((far - t // lows) * 4 + t % lows))

    def near_steps(act):
        for step in range(1, min(count, 4)):
            act(step)

    def load_orb(piece, half):
        cut = pl.ds((half * LOADS + piece) * span, span)
        return pltpu.make_async_copy(orb_hbm.at[:, cut], orb_line.at[:, cut], load_sem.at[piece])

    def loaded_orb(piece):
        cut = pl.ds(0, 2 * span)
        return pltpu.make_async_copy(orb_hbm.at[:, cut], orb_line.at[:, cut], load_sem.at[piece])

    def plane(ref, a):
        cut = pl.ds(pl.multiple_of(a * PLANE, PLANE), PLANE)
        return wide(ref[:, cut]).reshape(HALF, LANES)

    def remote_copy(src, dst, send, recv, peer):
        return pltpu.make_async_remote_copy(
            src_ref=src,
            dst_ref=dst,
            send_sem=send,
            recv_sem=recv,
            device_id={"band": peer},
            device_id_type=MESH,
        )

    def orbital(chunk):
        cut = pl.ds(chunk * depth, depth)
        return remote_copy(
            own_w.at[cut], remote.at[cut], send_sem.at[OWN], orb_recv.at[chunk], rem
        )

    to_sibling = remote_copy(own_w, sibling, send_sem.at[OWN], recv_sem.at[OWN], sib)
    own_sent = remote_copy(kern, field, send_sem.at[OWN], recv_sem.at[OWN], sib)

    def several(src, dst, kind, number):
        every = pl.ds(0, number)
        return remote_copy(
            src.at[every], dst.at[every], send_sem.at[kind], recv_sem.at[min(kind, PART)], sib
        )

    def trial_copy(step):
        peer = mate(step)
        return remote_copy(
            tri_rows.at[peer], t_in.at[me], send_sem.at[TRIAL], recv_sem.at[TRIAL], peer
        )

    def relay_copy(step, slot):
        return remote_copy(
            tri_rows.at[mate(step + 2)],
            r_in.at[slot],
            send_sem.at[TRIAL],
            r_recv.at[(step // 4 - 1) * 2 + step % 2],
            mate(step),
        )

    def onward(step):
        source = mate(step)
        return remote_copy(
            r_in.at[source], t_in.at[source], send_sem.at[ONWARD], recv_sem.at[TRIAL], mate(2)
        )

    def exchange_copy(step, slot):
        peer = mate(step)
        return remote_copy(
            e_rows.at[peer], e_in.at[slot], send_sem.at[EXCHANGE], e_recv.at[step - 1], peer
        )

    def part_copy(peer):
        return remote_copy(part, parts.at[me], send_sem.at[PART], recv_sem.at[PART], peer)

    def tile(group):
        return pl.ds(pl.multiple_of(group * TILE, TILE), TILE)

    def two(read, step):
        return jnp.concatenate([read(2 * step), read(2 * step + 1)], axis=1)

    def halved(value):
        lane = lax.broadcasted_iota(jnp.int32, (TILE, TILE), 1)
        return jnp.where(lane % LANES < LANES // 2, value[:TILE], value[TILE:])

    def rise(weighted, start, stop):
        @pl.loop(start // 2, stop // 2, unroll=min(UNROLL, (stop - start) // 2))
        def _(step):
            density = two(
                lambda group: low(wide(own[tile(group), :]) * wide(weighted[tile(group), :])), step
            )
            value = dot(left_b[...], low(dot(density, right_c[...])))
            field[tile(2 * step), :] = value[:, :LANES]
            field[tile(2 * step + 1), :] = value[:, LANES:]

    def strip(a, group):
        return pl.ds(pl.multiple_of(a * NG + group * SUB, SUB), SUB)

    def turn(unroll):
        @pl.loop(0, tiles // 2, unroll=unroll)
        def _(step):
            value = two(
                lambda group: low(
                    jnp.concatenate([field[strip(a, group), :] for a in range(HALF)], axis=0)
                ),
                step,
            )
            value = low(halved(dot(left_a[...], value)))
            value = low(wide(value) * two(lambda group: kern[tile(group), :], step))
            value = low(halved(dot(back_a[...], value)))
            value = dot(value, right_c[...])
            for side in range(2):
                for a in range(HALF):
                    field[strip(a, 2 * step + side), :] = value[
                        a * SUB : (a + 1) * SUB, side * LANES : (side + 1) * LANES
                    ]

    def fall(weighted, step):
        value = dot(left_b[...], two(lambda group: low(field[tile(group), :]), step))
        return [
            value[:, side * LANES : (side + 1) * LANES] * wide(weighted[tile(2 * step + side), :])
            for side in range(2)
        ]

    load_tables = pltpu.make_async_copy(tables_hbm, factors, load_sem.at[LOADS + 1])
    load_tri = pltpu.make_async_copy(tri_hbm, tri_line, load_sem.at[LOADS])

    def greet(i):
        pl.semaphore_signal(
            barrier, inc=1, device_id={"band": mate(i + 1)}, device_id_type=MESH
        )

    each(count, count - 1, lambda i: greet(count - 2 - i))

    for piece in range(LOADS):
        for half in range(2):
            load_orb(piece, half).start()
    load_tri.start()
    load_tables.start()

    fill = occ[0:1, :]
    for piece in range(LOADS):
        loaded_orb(piece).wait()

        @pl.loop(piece * HALF // LOADS, (piece + 1) * HALF // LOADS, unroll=2)
        def _(a):
            pair = jnp.concatenate(exchanged(plane(orb_line, a), plane(orb_line, a + HALF)), axis=0)
            cut = pl.ds(pl.multiple_of(a * NG, NG), NG)
            own[cut, :] = low(pair)
            own_w[cut, :] = low(pair * fill)


    load_tri.wait()

    @pl.loop(0, NG, unroll=2)
    def _(a):
        flat_t[pl.ds(pl.multiple_of(a * HALF, HALF), HALF), :] = low(plane(tri_line, a))

    load_tables.wait()
    pl.semaphore_wait(barrier, count - 1)
    for chunk in range(CHUNKS):
        orbital(chunk).start()
    to_sibling.start()

    trial_copy(1).start()

    def send_trial(step):
        relay_copy(step, me).start()
        trial_copy(step).start()

    far_first(2, send_trial)

    @pl.loop(0, tiles)
    def _(group):
        kern[tile(group), :] = screened_rows(group)

    rise(own_w, 0, tiles)
    turn(UNROLL)

    @pl.loop(0, tiles // 2, unroll=UNROLL)
    def _(step):
        for side, value in enumerate(fall(own_w, step)):
            acc[tile(2 * step + side), :] = value

    to_sibling.wait_recv()
    rise(sibling, 0, tiles)
    turn(UNROLL)

    @pl.loop(0, tiles // 2, unroll=UNROLL)
    def _(step):
        for side, value in enumerate(fall(sibling, step)):
            acc[tile(2 * step + side), :] += value

    for chunk in range(CHUNKS - 1):
        orbital(chunk).wait_recv()
        rise(remote, chunk * tiles // CHUNKS, (chunk + 1) * tiles // CHUNKS)
    orbital(CHUNKS - 1).wait_recv()
    for step in range(2, min(count, 4)):
        trial_copy(step).start()
    rise(remote, tiles - tiles // CHUNKS, tiles)
    turn(LAST_UNROLL)

    @pl.loop(0, tiles // 2, unroll=UNROLL)
    def _(step):
        for side, value in enumerate(fall(remote, step)):
            group = 2 * step + side
            value = -FRACTION * (acc[tile(group), :] + value)
            for j in range(per_tile):
                a = group * per_tile + j
                first, second = exchanged(
                    value[j * NG : j * NG + HALF], value[j * NG + HALF : (j + 1) * NG]
                )
                flat_e[pl.ds(pl.multiple_of(a * HALF, HALF), HALF), :] = low(first)
                flat_e[pl.ds(pl.multiple_of((a + HALF) * HALF, HALF), HALF), :] = low(second)

    t_in[pl.ds(me, 1)] = tri_rows[pl.ds(me, 1)]
    e_in[pl.ds(me, 1)] = e_rows[pl.ds(me, 1)]
    def send_exchange(step):
        exchange_copy(step, me).start()

    near_steps(send_exchange)
    far_steps(4, send_exchange)

    def spread_out(src, dst, slot):
        dst[pl.ds(slot, slab, stride=count), :] = wide(src[slot])

    def take_exchange(step):
        peer = mate(step)
        exchange_copy(step, peer).wait_recv()
        spread_out(e_in, et, peer)

    @pl.loop(0, NG, unroll=2)
    def _(a):
        cut = pl.ds(pl.multiple_of(a * PLANE, PLANE), PLANE)
        rows = wide(flat_e[pl.ds(pl.multiple_of(a * HALF, HALF), HALF), :])
        exch_line[:, cut] = low(rows.reshape(1, PLANE))

    store_line = pltpu.make_async_copy(exch_line, line_out, out_sem.at[0])
    store_low = pltpu.make_async_copy(et_low, low_out, out_sem.at[1])
    store_line.start()
    def pass_on(step):
        relay_copy(step, mate(step)).wait_recv()
        onward(step).start()

    far_first(2, pass_on)
    several(tri_rows, t_in, TRIAL, count - 1).wait_recv()

    @pl.loop(0, count, unroll=4)
    def _(slot):
        spread_out(t_in, et, slot)

    @pl.loop(0, tiles, unroll=4)
    def _(group):
        tt[tile(group), :] = low(et[tile(group), :])

    spread_out(e_in, et, me)
    near_steps(take_exchange)
    far_steps(4, take_exchange)

    mine = [low(et[r * count : (r + 1) * count, :]) for r in range(slab)]
    for r in range(slab):
        et_low[r * count : (r + 1) * count, :] = mine[r]
    total = lax.dot_general(
        jnp.concatenate([tt[r * count : (r + 1) * count, :] for r in range(slab)], axis=1),
        jnp.concatenate(mine, axis=1),
        (((1,), (1,)), ((), ())),
        preferred_element_type=jnp.float32,
    )
    if spread > 1:
        rest = jnp.zeros((count, LANES - count), jnp.float32)
        total = grown(jnp.concatenate([total, rest], axis=1), count)
    if spread > 1:
        total = jnp.sum(
            jnp.where(own_lanes(count), total, 0.0).reshape(count // spread, spread, LANES), axis=1
        )
    part[...] = total
    parts[pl.ds(me, 1)] = total[None]

    def send_part(peer):
        @pl.when(peer != me)
        def _():
            part_copy(peer).start()

    each(count, count, send_part)
    store_low.start()
    own_sent.wait_send()
    several(tri_rows, t_in, TRIAL, count - 1).wait_send()
    if far > 0:
        several(r_in, t_in, ONWARD, 2 * far).wait_send()
    several(e_rows, e_in, EXCHANGE, count - 1).wait_send()
    store_line.wait()
    store_low.wait()
    several(parts, parts, PART, count - 1).wait()
    total_here[...] = jnp.sum(parts[...], axis=0)
    store_sum = pltpu.make_async_copy(total_here, summed, out_sem.at[2])
    store_sum.start()
    store_sum.wait()


def finish(count, exch_line, et_low, summed, exch_hbm, proj_hbm, proj, out_sem):
    pack = TILE // count
    spread = LANES // count
    groups = ROWS // TILE
    width = pack * LANES
    stores = []
    part = exch_line.shape[1] // PIECES
    for piece in range(PIECES):
        cut = pl.ds(piece * part, part)
        stores.append(
            pltpu.make_async_copy(
                exch_line.at[:, cut], exch_hbm.at[:, cut], out_sem.at[groups + piece]
            )
        )
        stores[-1].start()
    total = summed[...] / math.sqrt(ROWS * LANES)
    if spread > 1:
        total = jnp.broadcast_to(total[:, None, :], (count // spread, spread, LANES))
        total = jnp.where(own_lanes(count), total.reshape(count, LANES), 0.0)
    total = grown(total, count)
    mixing = low(total[:, :count])
    for group in range(groups):
        for r in range(0, pack, 2):
            row = (group * pack + r) * count
            at = (group * pack + r) * LANES
            sides = [et_low[row + k * count : row + (k + 1) * count, :] for k in range(2)]
            piece = dot(mixing, jnp.concatenate(sides, axis=1))
            proj[:, at : at + 2 * LANES] = low(piece * (-1.0 / math.sqrt(count)))
        cut = pl.ds(group * width, width)
        stores.append(
            pltpu.make_async_copy(proj.at[:, cut], proj_hbm.at[:, cut], out_sem.at[group])
        )
        stores[-1].start()
    for store in stores:
        store.wait()


def local(orbitals, trial, occupations):
    count = lax.axis_size("band")
    cells = orbitals.shape[1]
    slab = ROWS // count
    rows = (ROWS, LANES)
    bf16, f32 = jnp.bfloat16, jnp.float32
    compact = (count // (LANES // count), LANES)
    dma = pltpu.SemaphoreType.DMA
    anywhere = pl.BlockSpec(memory_space=pl.ANY)
    vmem = pl.BlockSpec(memory_space=pltpu.VMEM)
    consts = tables()
    line, spread_low, summed = pl.pallas_call(
        functools.partial(body, count),
        out_shape=(
            jax.ShapeDtypeStruct((1, cells), bf16),
            jax.ShapeDtypeStruct(rows, bf16),
            jax.ShapeDtypeStruct(compact, f32),
        ),
        in_specs=[pl.BlockSpec(memory_space=pltpu.HBM)] * 3 + [vmem],
        out_specs=(anywhere, anywhere, anywhere),
        scratch_shapes=[
            pltpu.VMEM(consts.shape, bf16),
            pltpu.VMEM((1, cells), bf16),
            pltpu.VMEM((1, cells), bf16),
            pltpu.VMEM(rows, bf16),
            pltpu.VMEM(rows, bf16),
            pltpu.VMEM(rows, bf16),
            pltpu.VMEM(rows, bf16),
            pltpu.VMEM((count, slab, LANES), bf16),
            pltpu.VMEM(rows, f32),
            pltpu.VMEM(rows, f32),
            pltpu.VMEM(rows, f32),
            pltpu.VMEM((count, slab, LANES), bf16),
            pltpu.VMEM((count, slab, LANES), bf16),
            pltpu.VMEM((count, slab, LANES), bf16),
            pltpu.VMEM((count, slab, LANES), bf16),
            pltpu.VMEM(rows, bf16),
            pltpu.VMEM(rows, f32),
            pltpu.VMEM((1, cells), bf16),
            pltpu.VMEM(rows, bf16),
            pltpu.VMEM(compact, f32),
            pltpu.VMEM((count,) + compact, f32),
            pltpu.VMEM(compact, f32),
            dma((LOADS + 2,)),
            dma((5,)),
            dma((3,)),
            dma((CHUNKS,)),
            dma((max(2 * (count // 4 - 1), 1),)),
            dma((count - 1,)),
            dma((3,)),
        ],
        compiler_params=pltpu.CompilerParams(
            collective_id=1, has_side_effects=True, vmem_limit_bytes=VMEM_LIMIT
        ),
        name="exchange",
    )(
        *[pltpu.with_memory_space_constraint(x, pltpu.HBM) for x in (orbitals, trial, consts)],
        jnp.broadcast_to(occupations.astype(f32)[:, None], (8, LANES)),
    )
    return pl.pallas_call(
        functools.partial(finish, count),
        out_shape=(
            jax.ShapeDtypeStruct((1, cells), bf16),
            jax.ShapeDtypeStruct((count, cells // count), bf16),
        ),
        in_specs=[vmem, vmem, vmem],
        out_specs=(anywhere, anywhere),
        scratch_shapes=[
            pltpu.VMEM((count, cells // count), bf16),
            dma((ROWS // TILE + PIECES,)),
        ],
        compiler_params=pltpu.CompilerParams(vmem_limit_bytes=VMEM_LIMIT),
        name="finish",
    )(line, spread_low, summed)


def solution(mesh):
    return jax.shard_map(
        local,
        mesh=mesh,
        in_specs=(P(("spin", "band"), None), P(("spin", "band"), None), P(("spin", "band"))),
        out_specs=(P(("spin", "band"), None), P("spin", "band")),
        check_vma=False,
    )
```

```python
import functools
import math

import jax
import jax.numpy as jnp
import numpy as np
from jax import lax
from jax.experimental import pallas as pl
from jax.experimental.pallas import tpu as pltpu
from jax.sharding import PartitionSpec as P

NG = 64
FRACTION = 0.25
OMEGA = 1.0
LANES = 128
TILE = 256
CHUNKS = 4
UNROLL = 2
LAST_UNROLL = 2
VMEM_LIMIT = 30 << 20
WRITTEN_OUT = 32
PIECES = 1
LOADS = 2
OWN, TRIAL, PART, ONWARD, EXCHANGE = range(5)
MESH = pl.DeviceIdType.MESH

HALF = NG // 2
SUB = TILE // HALF
PLANE = NG * NG
ROWS = NG * NG * NG // LANES


def cas_table():
    index = np.arange(NG)
    phases = (index[:, None] * index[None, :] % NG).astype(np.float32) * np.float32(2.0 * math.pi / NG)
    return np.cos(phases) + np.sin(phases)


def tables():
    table = cas_table()
    order = np.concatenate([np.arange(0, NG, 2), np.arange(1, NG, 2)])
    eye = np.eye(TILE // NG, dtype=np.float32)
    sums = np.array([[1.0, 1.0], [1.0, -1.0]], np.float32)
    right_c = np.kron(np.eye(TILE // LANES, dtype=np.float32), np.kron(sums, table))
    left_b = np.kron(eye, table[order][:, order])
    halves = (table[0::2, :HALF], table[1::2, :HALF])
    rows = np.eye(TILE // HALF, dtype=np.float32)
    left_a = np.concatenate([np.kron(half, rows) for half in halves])
    back_a = np.concatenate([np.kron(half.T, rows) for half in halves])
    return jnp.asarray(np.concatenate([left_a, back_a, left_b, right_c])).astype(jnp.bfloat16)


def dot(left, right):
    return jnp.dot(left, right, preferred_element_type=jnp.float32)


def low(value):
    return value.astype(jnp.bfloat16)


def wide(value):
    return value.astype(jnp.float32)


def exchanged(first, second):
    lower = lax.broadcasted_iota(jnp.int32, first.shape, 1) < LANES // 2
    return (
        jnp.where(lower, first, pltpu.roll(second, LANES // 2, 1)),
        jnp.where(lower, pltpu.roll(first, LANES // 2, 1), second),
    )


def wavenum_sq(index):
    modes = wide(jnp.where(2 * index < NG, index, index - NG))
    wavenum = modes * (2.0 * math.pi / NG)
    return wavenum * wavenum


def screened_rows(group):
    shape = (TILE, LANES)
    row = lax.broadcasted_iota(jnp.int32, shape, 0)
    lane = lax.broadcasted_iota(jnp.int32, shape, 1)
    a = 2 * (row // SUB) + lane // NG
    place = group * SUB + row % SUB
    b = 2 * (place % HALF) + place // HALF
    norm_sq = wavenum_sq(a) + wavenum_sq(b) + wavenum_sq(lane % NG)
    bounded = jnp.where(norm_sq > 0, norm_sq, 1.0)
    screened = jnp.where(
        norm_sq > 0,
        4.0 * math.pi / bounded * (1.0 - jnp.exp(-bounded / (4.0 * OMEGA * OMEGA))),
        math.pi / (OMEGA * OMEGA),
    )
    return screened * (1.0 / NG**3)


def partner(me, step, count):
    total, bit = 0, 1
    while bit < count:
        total = total + bit * ((me // bit + step // bit) % 2)
        bit *= 2
    return total


def each(count, number, act):
    if count <= WRITTEN_OUT:
        for i in range(number):
            act(i)
    else:
        pl.loop(0, number)(act)


def grown(total, count):
    shift = LANES // 2
    while shift >= count:
        total = total + pltpu.roll(total, shift, 1)
        shift //= 2
    return total


def own_lanes(count):
    shape = (count, LANES)
    spread = LANES // count
    return (
        lax.broadcasted_iota(jnp.int32, shape, 0) % spread
        == lax.broadcasted_iota(jnp.int32, shape, 1) // count
    )


def body(
    count,
    orb_hbm, tri_hbm, tables_hbm, occ,
    line_out, low_out, summed,
    factors,
    orb_line, tri_line, own, own_w, sibling, remote, tri_rows, kern, field, acc,
    e_rows, t_in, r_in, e_in, tt, et, exch_line, et_low, part, parts, total_here,
    load_sem, send_sem, recv_sem, orb_recv, r_recv, e_recv, out_sem,
):
    me = lax.axis_index("band")
    flips = [bit * (1 - 2 * (me // bit % 2)) for bit in (1 << k for k in range(count.bit_length() - 1))]

    def mate(step):
        if isinstance(step, int):
            return me + sum(flip for k, flip in enumerate(flips) if step >> k & 1)
        return partner(me, step, count)

    barrier = pltpu.get_barrier_semaphore()
    slab = ROWS // count
    spread = LANES // count
    tiles = ROWS // TILE
    per_tile = TILE // NG
    depth = ROWS // CHUNKS
    span = HALF // LOADS * PLANE
    planes = max(count // 4, 1)
    sib = me + 1 - 2 * (me % 2)
    rem = (me + count - 1 + 2 * (me % 2)) % count
    left_a = factors.at[: 2 * TILE]
    back_a = factors.at[2 * TILE : 4 * TILE]
    left_b = factors.at[4 * TILE : 5 * TILE]
    right_c = factors.at[5 * TILE :]
    flat_t = tri_rows.reshape(ROWS, LANES)
    flat_e = e_rows.reshape(ROWS, LANES)

    far = planes - 1

    def far_steps(lows, act):
        def mixed(t):
            upper = t % far
            act((1 + upper) * 4 + (t // far + 2 * upper) % lows)

        each(count, lows * far, mixed)

    def far_first(lows, act):
        each(count, lows * far, lambda t: act((far - t // lows) * 4 + t % lows))

    def near_steps(act):
        for step in range(1, min(count, 4)):
            act(step)

    def load_orb(piece, half):
        cut = pl.ds((half * LOADS + piece) * span, span)
        return pltpu.make_async_copy(orb_hbm.at[:, cut], orb_line.at[:, cut], load_sem.at[piece])

    def loaded_orb(piece):
        cut = pl.ds(0, 2 * span)
        return pltpu.make_async_copy(orb_hbm.at[:, cut], orb_line.at[:, cut], load_sem.at[piece])

    def plane(ref, a):
        cut = pl.ds(pl.multiple_of(a * PLANE, PLANE), PLANE)
        return wide(ref[:, cut]).reshape(HALF, LANES)

    def remote_copy(src, dst, send, recv, peer):
        return pltpu.make_async_remote_copy(
            src_ref=src,
            dst_ref=dst,
            send_sem=send,
            recv_sem=recv,
            device_id={"band": peer},
            device_id_type=MESH,
        )

    def orbital(chunk):
        cut = pl.ds(chunk * depth, depth)
        return remote_copy(
            own_w.at[cut], remote.at[cut], send_sem.at[OWN], orb_recv.at[chunk], rem
        )

    to_sibling = remote_copy(own_w, sibling, send_sem.at[OWN], recv_sem.at[OWN], sib)
    own_sent = remote_copy(kern, field, send_sem.at[OWN], recv_sem.at[OWN], sib)

    def several(src, dst, kind, number):
        every = pl.ds(0, number)
        return remote_copy(
            src.at[every], dst.at[every], send_sem.at[kind], recv_sem.at[min(kind, PART)], sib
        )

    def trial_copy(step):
        peer = mate(step)
        return remote_copy(
            tri_rows.at[peer], t_in.at[me], send_sem.at[TRIAL], recv_sem.at[TRIAL], peer
        )

    def relay_copy(step, slot):
        return remote_copy(
            tri_rows.at[mate(step + 2)],
            r_in.at[slot],
            send_sem.at[TRIAL],
            r_recv.at[(step // 4 - 1) * 2 + step % 2],
            mate(step),
        )

    def onward(step):
        source = mate(step)
        return remote_copy(
            r_in.at[source], t_in.at[source], send_sem.at[ONWARD], recv_sem.at[TRIAL], mate(2)
        )

    def exchange_copy(step, slot):
        peer = mate(step)
        return remote_copy(
            e_rows.at[peer], e_in.at[slot], send_sem.at[EXCHANGE], e_recv.at[step - 1], peer
        )

    def part_copy(peer):
        return remote_copy(part, parts.at[me], send_sem.at[PART], recv_sem.at[PART], peer)

    def tile(group):
        return pl.ds(pl.multiple_of(group * TILE, TILE), TILE)

    def two(read, step):
        return jnp.concatenate([read(2 * step), read(2 * step + 1)], axis=1)

    def halved(value):
        lane = lax.broadcasted_iota(jnp.int32, (TILE, TILE), 1)
        return jnp.where(lane % LANES < LANES // 2, value[:TILE], value[TILE:])

    def rise(weighted, start, stop):
        @pl.loop(start // 2, stop // 2, unroll=min(UNROLL, (stop - start) // 2))
        def _(step):
            density = two(
                lambda group: low(wide(own[tile(group), :]) * wide(weighted[tile(group), :])), step
            )
            value = dot(left_b[...], low(dot(density, right_c[...])))
            field[tile(2 * step), :] = value[:, :LANES]
            field[tile(2 * step + 1), :] = value[:, LANES:]

    def strip(a, group):
        return pl.ds(pl.multiple_of(a * NG + group * SUB, SUB), SUB)

    def turn(unroll):
        @pl.loop(0, tiles // 2, unroll=unroll)
        def _(step):
            value = two(
                lambda group: low(
                    jnp.concatenate([field[strip(a, group), :] for a in range(HALF)], axis=0)
                ),
                step,
            )
            value = low(halved(dot(left_a[...], value)))
            value = low(wide(value) * two(lambda group: kern[tile(group), :], step))
            value = low(halved(dot(back_a[...], value)))
            value = dot(value, right_c[...])
            for side in range(2):
                for a in range(HALF):
                    field[strip(a, 2 * step + side), :] = value[
                        a * SUB : (a + 1) * SUB, side * LANES : (side + 1) * LANES
                    ]

    def fall(weighted, step):
        value = dot(left_b[...], two(lambda group: low(field[tile(group), :]), step))
        return [
            value[:, side * LANES : (side + 1) * LANES] * wide(weighted[tile(2 * step + side), :])
            for side in range(2)
        ]

    load_tables = pltpu.make_async_copy(tables_hbm, factors, load_sem.at[LOADS + 1])
    load_tri = pltpu.make_async_copy(tri_hbm, tri_line, load_sem.at[LOADS])

    def greet(i):
        pl.semaphore_signal(
            barrier, inc=1, device_id={"band": mate(i + 1)}, device_id_type=MESH
        )

    each(count, count - 1, lambda i: greet(count - 2 - i))

    for piece in range(LOADS):
        for half in range(2):
            load_orb(piece, half).start()
    load_tri.start()
    load_tables.start()

    fill = occ[0:1, :]
    for piece in range(LOADS):
        loaded_orb(piece).wait()

        @pl.loop(piece * HALF // LOADS, (piece + 1) * HALF // LOADS, unroll=2)
        def _(a):
            pair = jnp.concatenate(exchanged(plane(orb_line, a), plane(orb_line, a + HALF)), axis=0)
            cut = pl.ds(pl.multiple_of(a * NG, NG), NG)
            own[cut, :] = low(pair)
            own_w[cut, :] = low(pair * fill)


    load_tri.wait()

    @pl.loop(0, NG, unroll=2)
    def _(a):
        flat_t[pl.ds(pl.multiple_of(a * HALF, HALF), HALF), :] = low(plane(tri_line, a))

    load_tables.wait()
    pl.semaphore_wait(barrier, count - 1)
    for chunk in range(CHUNKS):
        orbital(chunk).start()
    to_sibling.start()

    trial_copy(1).start()

    def send_trial(step):
        relay_copy(step, me).start()
        trial_copy(step).start()

    if far > 0:
        for low_bit in range(2):
            send_trial(far * 4 + low_bit)

    @pl.loop(0, tiles)
    def _(group):
        kern[tile(group), :] = screened_rows(group)

    rise(own_w, 0, tiles)
    turn(UNROLL)

    @pl.loop(0, tiles // 2, unroll=UNROLL)
    def _(step):
        for side, value in enumerate(fall(own_w, step)):
            acc[tile(2 * step + side), :] = value

    each(count, 2 * (far - 1), lambda t: send_trial((far - 1 - t // 2) * 4 + t % 2))
    to_sibling.wait_recv()
    rise(sibling, 0, tiles)
    turn(UNROLL)

    @pl.loop(0, tiles // 2, unroll=UNROLL)
    def _(step):
        for side, value in enumerate(fall(sibling, step)):
            acc[tile(2 * step + side), :] += value

    for chunk in range(CHUNKS - 1):
        orbital(chunk).wait_recv()
        rise(remote, chunk * tiles // CHUNKS, (chunk + 1) * tiles // CHUNKS)
    orbital(CHUNKS - 1).wait_recv()
    for step in range(2, min(count, 4)):
        trial_copy(step).start()
    rise(remote, tiles - tiles // CHUNKS, tiles)
    turn(LAST_UNROLL)

    @pl.loop(0, tiles // 2, unroll=UNROLL)
    def _(step):
        for side, value in enumerate(fall(remote, step)):
            group = 2 * step + side
            value = -FRACTION * (acc[tile(group), :] + value)
            for j in range(per_tile):
                a = group * per_tile + j
                first, second = exchanged(
                    value[j * NG : j * NG + HALF], value[j * NG + HALF : (j + 1) * NG]
                )
                flat_e[pl.ds(pl.multiple_of(a * HALF, HALF), HALF), :] = low(first)
                flat_e[pl.ds(pl.multiple_of((a + HALF) * HALF, HALF), HALF), :] = low(second)

    t_in[pl.ds(me, 1)] = tri_rows[pl.ds(me, 1)]
    e_in[pl.ds(me, 1)] = e_rows[pl.ds(me, 1)]
    def send_exchange(step):
        exchange_copy(step, me).start()

    near_steps(send_exchange)
    far_steps(4, send_exchange)

    def spread_out(src, dst, slot):
        dst[pl.ds(slot, slab, stride=count), :] = wide(src[slot])

    def take_exchange(step):
        peer = mate(step)
        exchange_copy(step, peer).wait_recv()
        spread_out(e_in, et, peer)

    @pl.loop(0, NG, unroll=2)
    def _(a):
        cut = pl.ds(pl.multiple_of(a * PLANE, PLANE), PLANE)
        rows = wide(flat_e[pl.ds(pl.multiple_of(a * HALF, HALF), HALF), :])
        exch_line[:, cut] = low(rows.reshape(1, PLANE))

    store_line = pltpu.make_async_copy(exch_line, line_out, out_sem.at[0])
    store_low = pltpu.make_async_copy(et_low, low_out, out_sem.at[1])
    store_line.start()
    def pass_on(step):
        relay_copy(step, mate(step)).wait_recv()
        onward(step).start()

    far_steps(2, pass_on)
    several(tri_rows, t_in, TRIAL, count - 1).wait_recv()

    @pl.loop(0, count, unroll=4)
    def _(slot):
        spread_out(t_in, et, slot)

    @pl.loop(0, tiles, unroll=4)
    def _(group):
        tt[tile(group), :] = low(et[tile(group), :])

    spread_out(e_in, et, me)
    near_steps(take_exchange)
    far_steps(4, take_exchange)

    mine = [low(et[r * count : (r + 1) * count, :]) for r in range(slab)]
    for r in range(slab):
        et_low[r * count : (r + 1) * count, :] = mine[r]
    total = lax.dot_general(
        jnp.concatenate([tt[r * count : (r + 1) * count, :] for r in range(slab)], axis=1),
        jnp.concatenate(mine, axis=1),
        (((1,), (1,)), ((), ())),
        preferred_element_type=jnp.float32,
    )
    if spread > 1:
        rest = jnp.zeros((count, LANES - count), jnp.float32)
        total = jnp.concatenate([total, rest], axis=1)
        total = pltpu.roll(total, 0, 1, stride=count, stride_axis=0)
        total = jnp.sum(total.reshape(count // spread, spread, LANES), axis=1)
    part[...] = total
    parts[pl.ds(me, 1)] = total[None]

    def send_part(peer):
        @pl.when(peer != me)
        def _():
            part_copy(peer).start()

    each(count, count, send_part)
    store_low.start()
    own_sent.wait_send()
    several(tri_rows, t_in, TRIAL, count - 1).wait_send()
    if far > 0:
        several(r_in, t_in, ONWARD, 2 * far).wait_send()
    several(e_rows, e_in, EXCHANGE, count - 1).wait_send()
    store_line.wait()
    store_low.wait()
    several(parts, parts, PART, count - 1).wait()
    total_here[...] = jnp.sum(parts[...], axis=0)
    store_sum = pltpu.make_async_copy(total_here, summed, out_sem.at[2])
    store_sum.start()
    store_sum.wait()


def finish(count, exch_line, et_low, summed, exch_hbm, proj_hbm, proj, out_sem):
    pack = TILE // count
    spread = LANES // count
    groups = ROWS // TILE
    width = pack * LANES
    stores = []
    part = exch_line.shape[1] // PIECES
    for piece in range(PIECES):
        cut = pl.ds(piece * part, part)
        stores.append(
            pltpu.make_async_copy(
                exch_line.at[:, cut], exch_hbm.at[:, cut], out_sem.at[groups // 2 + piece]
            )
        )
        stores[-1].start()
    total = summed[...] / math.sqrt(ROWS * LANES)
    if spread > 1:
        total = jnp.broadcast_to(total[:, None, :], (count // spread, spread, LANES))
        total = jnp.where(own_lanes(count), total.reshape(count, LANES), 0.0)
    total = grown(total, count)
    mixing = low(total[:, :count])
    for group in range(groups):
        for r in range(0, pack, 2):
            row = (group * pack + r) * count
            at = (group * pack + r) * LANES
            sides = [et_low[row + k * count : row + (k + 1) * count, :] for k in range(2)]
            piece = dot(mixing, jnp.concatenate(sides, axis=1))
            proj[:, at : at + 2 * LANES] = low(piece * (-1.0 / math.sqrt(count)))
        if group % 2 == 1:
            cut = pl.ds((group - 1) * width, 2 * width)
            stores.append(
                pltpu.make_async_copy(proj.at[:, cut], proj_hbm.at[:, cut], out_sem.at[group // 2])
            )
            stores[-1].start()
    for store in stores:
        store.wait()


def local(orbitals, trial, occupations):
    count = lax.axis_size("band")
    cells = orbitals.shape[1]
    slab = ROWS // count
    rows = (ROWS, LANES)
    bf16, f32 = jnp.bfloat16, jnp.float32
    compact = (count // (LANES // count), LANES)
    dma = pltpu.SemaphoreType.DMA
    anywhere = pl.BlockSpec(memory_space=pl.ANY)
    vmem = pl.BlockSpec(memory_space=pltpu.VMEM)
    consts = tables()
    line, spread_low, summed = pl.pallas_call(
        functools.partial(body, count),
        out_shape=(
            jax.ShapeDtypeStruct((1, cells), bf16),
            jax.ShapeDtypeStruct(rows, bf16),
            jax.ShapeDtypeStruct(compact, f32),
        ),
        in_specs=[pl.BlockSpec(memory_space=pltpu.HBM)] * 3 + [vmem],
        out_specs=(anywhere, anywhere, anywhere),
        scratch_shapes=[
            pltpu.VMEM(consts.shape, bf16),
            pltpu.VMEM((1, cells), bf16),
            pltpu.VMEM((1, cells), bf16),
            pltpu.VMEM(rows, bf16),
            pltpu.VMEM(rows, bf16),
            pltpu.VMEM(rows, bf16),
            pltpu.VMEM(rows, bf16),
            pltpu.VMEM((count, slab, LANES), bf16),
            pltpu.VMEM(rows, f32),
            pltpu.VMEM(rows, f32),
            pltpu.VMEM(rows, f32),
            pltpu.VMEM((count, slab, LANES), bf16),
            pltpu.VMEM((count, slab, LANES), bf16),
            pltpu.VMEM((count, slab, LANES), bf16),
            pltpu.VMEM((count, slab, LANES), bf16),
            pltpu.VMEM(rows, bf16),
            pltpu.VMEM(rows, f32),
            pltpu.VMEM((1, cells), bf16),
            pltpu.VMEM(rows, bf16),
            pltpu.VMEM(compact, f32),
            pltpu.VMEM((count,) + compact, f32),
            pltpu.VMEM(compact, f32),
            dma((LOADS + 2,)),
            dma((5,)),
            dma((3,)),
            dma((CHUNKS,)),
            dma((max(2 * (count // 4 - 1), 1),)),
            dma((count - 1,)),
            dma((3,)),
        ],
        compiler_params=pltpu.CompilerParams(
            collective_id=1, has_side_effects=True, vmem_limit_bytes=VMEM_LIMIT
        ),
        name="exchange",
    )(
        *[pltpu.with_memory_space_constraint(x, pltpu.HBM) for x in (orbitals, trial, consts)],
        jnp.broadcast_to(occupations.astype(f32)[:, None], (8, LANES)),
    )
    return pl.pallas_call(
        functools.partial(finish, count),
        out_shape=(
            jax.ShapeDtypeStruct((1, cells), bf16),
            jax.ShapeDtypeStruct((count, cells // count), bf16),
        ),
        in_specs=[vmem, vmem, vmem],
        out_specs=(anywhere, anywhere),
        scratch_shapes=[
            pltpu.VMEM((count, cells // count), bf16),
            dma((ROWS // TILE // 2 + PIECES,)),
        ],
        compiler_params=pltpu.CompilerParams(vmem_limit_bytes=VMEM_LIMIT),
        name="finish",
    )(line, spread_low, summed)


def solution(mesh):
    return jax.shard_map(
        local,
        mesh=mesh,
        in_specs=(P(("spin", "band"), None), P(("spin", "band"), None), P(("spin", "band"))),
        out_specs=(P(("spin", "band"), None), P("spin", "band")),
        check_vma=False,
    )
```

```python
import functools
import math

import jax
import jax.numpy as jnp
import numpy as np
from jax import lax
from jax.experimental import pallas as pl
from jax.experimental.pallas import tpu as pltpu
from jax.sharding import PartitionSpec as P

NG = 64
FRACTION = 0.25
OMEGA = 1.0
LANES = 128
TILE = 256
CHUNKS = 4
UNROLL = 2
LAST_UNROLL = 2
VMEM_LIMIT = 30 << 20
WRITTEN_OUT = 32
PIECES = 1
LOADS = 2
OWN, TRIAL, PART, ONWARD, EXCHANGE = range(5)
MESH = pl.DeviceIdType.MESH

HALF = NG // 2
SUB = TILE // HALF
PLANE = NG * NG
ROWS = NG * NG * NG // LANES


def cas_table():
    index = np.arange(NG)
    phases = (index[:, None] * index[None, :] % NG).astype(np.float32) * np.float32(2.0 * math.pi / NG)
    return np.cos(phases) + np.sin(phases)


def tables():
    table = cas_table()
    order = np.concatenate([np.arange(0, NG, 2), np.arange(1, NG, 2)])
    eye = np.eye(TILE // NG, dtype=np.float32)
    sums = np.array([[1.0, 1.0], [1.0, -1.0]], np.float32)
    right_c = np.kron(np.eye(TILE // LANES, dtype=np.float32), np.kron(sums, table))
    left_b = np.kron(eye, table[order][:, order])
    halves = (table[0::2, :HALF], table[1::2, :HALF])
    rows = np.eye(TILE // HALF, dtype=np.float32)
    left_a = np.concatenate([np.kron(half, rows) for half in halves])
    back_a = np.concatenate([np.kron(half.T, rows) for half in halves])
    return jnp.asarray(np.concatenate([left_a, back_a, left_b, right_c])).astype(jnp.bfloat16)


def dot(left, right):
    return jnp.dot(left, right, preferred_element_type=jnp.float32)


def low(value):
    return value.astype(jnp.bfloat16)


def wide(value):
    return value.astype(jnp.float32)


def exchanged(first, second):
    lower = lax.broadcasted_iota(jnp.int32, first.shape, 1) < LANES // 2
    return (
        jnp.where(lower, first, pltpu.roll(second, LANES // 2, 1)),
        jnp.where(lower, pltpu.roll(first, LANES // 2, 1), second),
    )


def wavenum_sq(index):
    modes = wide(jnp.where(2 * index < NG, index, index - NG))
    wavenum = modes * (2.0 * math.pi / NG)
    return wavenum * wavenum


def screened_rows(group):
    shape = (TILE, LANES)
    row = lax.broadcasted_iota(jnp.int32, shape, 0)
    lane = lax.broadcasted_iota(jnp.int32, shape, 1)
    a = 2 * (row // SUB) + lane // NG
    place = group * SUB + row % SUB
    b = 2 * (place % HALF) + place // HALF
    norm_sq = wavenum_sq(a) + wavenum_sq(b) + wavenum_sq(lane % NG)
    bounded = jnp.where(norm_sq > 0, norm_sq, 1.0)
    screened = jnp.where(
        norm_sq > 0,
        4.0 * math.pi / bounded * (1.0 - jnp.exp(-bounded / (4.0 * OMEGA * OMEGA))),
        math.pi / (OMEGA * OMEGA),
    )
    return screened * (1.0 / NG**3)


def partner(me, step, count):
    total, bit = 0, 1
    while bit < count:
        total = total + bit * ((me // bit + step // bit) % 2)
        bit *= 2
    return total


def each(count, number, act):
    if count <= WRITTEN_OUT:
        for i in range(number):
            act(i)
    else:
        pl.loop(0, number)(act)


def grown(total, count):
    shift = LANES // 2
    while shift >= count:
        total = total + pltpu.roll(total, shift, 1)
        shift //= 2
    return total


def own_lanes(count):
    shape = (count, LANES)
    spread = LANES // count
    return (
        lax.broadcasted_iota(jnp.int32, shape, 0) % spread
        == lax.broadcasted_iota(jnp.int32, shape, 1) // count
    )


def body(
    count,
    orb_hbm, tri_hbm, tables_hbm, occ,
    line_out, low_out, summed,
    factors,
    orb_line, tri_line, own, own_w, sibling, remote, tri_rows, kern, field, acc,
    e_rows, t_in, r_in, e_in, tt, et, exch_line, et_low, part, parts, total_here,
    load_sem, send_sem, recv_sem, orb_recv, r_recv, e_recv, out_sem,
):
    me = lax.axis_index("band")
    flips = [bit * (1 - 2 * (me // bit % 2)) for bit in (1 << k for k in range(count.bit_length() - 1))]

    def mate(step):
        if isinstance(step, int):
            return me + sum(flip for k, flip in enumerate(flips) if step >> k & 1)
        return partner(me, step, count)

    barrier = pltpu.get_barrier_semaphore()
    slab = ROWS // count
    spread = LANES // count
    tiles = ROWS // TILE
    per_tile = TILE // NG
    depth = ROWS // CHUNKS
    span = HALF // LOADS * PLANE
    planes = max(count // 4, 1)
    sib = me + 1 - 2 * (me % 2)
    rem = (me + count - 1 + 2 * (me % 2)) % count
    left_a = factors.at[: 2 * TILE]
    back_a = factors.at[2 * TILE : 4 * TILE]
    left_b = factors.at[4 * TILE : 5 * TILE]
    right_c = factors.at[5 * TILE :]
    flat_t = tri_rows.reshape(ROWS, LANES)
    flat_e = e_rows.reshape(ROWS, LANES)

    far = planes - 1

    def far_steps(lows, act):
        def mixed(t):
            upper = t % far
            act((1 + upper) * 4 + (t // far + 2 * upper) % lows)

        each(count, lows * far, mixed)

    def far_first(lows, act):
        each(count, lows * far, lambda t: act((far - t // lows) * 4 + t % lows))

    def near_steps(act):
        for step in range(1, min(count, 4)):
            act(step)

    def load_orb(piece, half):
        cut = pl.ds((half * LOADS + piece) * span, span)
        return pltpu.make_async_copy(orb_hbm.at[:, cut], orb_line.at[:, cut], load_sem.at[piece])

    def loaded_orb(piece):
        cut = pl.ds(0, 2 * span)
        return pltpu.make_async_copy(orb_hbm.at[:, cut], orb_line.at[:, cut], load_sem.at[piece])

    def plane(ref, a):
        cut = pl.ds(pl.multiple_of(a * PLANE, PLANE), PLANE)
        return wide(ref[:, cut]).reshape(HALF, LANES)

    def remote_copy(src, dst, send, recv, peer):
        return pltpu.make_async_remote_copy(
            src_ref=src,
            dst_ref=dst,
            send_sem=send,
            recv_sem=recv,
            device_id={"band": peer},
            device_id_type=MESH,
        )

    def orbital(chunk):
        cut = pl.ds(chunk * depth, depth)
        return remote_copy(
            own_w.at[cut], remote.at[cut], send_sem.at[OWN], orb_recv.at[chunk], rem
        )

    to_sibling = remote_copy(own_w, sibling, send_sem.at[OWN], recv_sem.at[OWN], sib)
    own_sent = remote_copy(kern, field, send_sem.at[OWN], recv_sem.at[OWN], sib)

    def several(src, dst, kind, number):
        every = pl.ds(0, number)
        return remote_copy(
            src.at[every], dst.at[every], send_sem.at[kind], recv_sem.at[min(kind, PART)], sib
        )

    def trial_copy(step):
        peer = mate(step)
        return remote_copy(
            tri_rows.at[peer], t_in.at[me], send_sem.at[TRIAL], recv_sem.at[TRIAL], peer
        )

    def relay_copy(step, slot):
        return remote_copy(
            tri_rows.at[mate(step + 2)],
            r_in.at[slot],
            send_sem.at[TRIAL],
            r_recv.at[step // 4 - 1],
            mate(step),
        )

    def onward(step):
        source = mate(step)
        return remote_copy(
            r_in.at[source], t_in.at[source], send_sem.at[ONWARD], recv_sem.at[TRIAL], mate(2)
        )

    def exchange_copy(step, slot):
        peer = mate(step)
        return remote_copy(
            e_rows.at[peer], e_in.at[slot], send_sem.at[EXCHANGE], e_recv.at[step - 1], peer
        )

    def part_copy(peer):
        return remote_copy(part, parts.at[me], send_sem.at[PART], recv_sem.at[PART], peer)

    def tile(group):
        return pl.ds(pl.multiple_of(group * TILE, TILE), TILE)

    def two(read, step):
        return jnp.concatenate([read(2 * step), read(2 * step + 1)], axis=1)

    def halved(value):
        lane = lax.broadcasted_iota(jnp.int32, (TILE, TILE), 1)
        return jnp.where(lane % LANES < LANES // 2, value[:TILE], value[TILE:])

    def rise(weighted, start, stop):
        @pl.loop(start // 2, stop // 2, unroll=min(UNROLL, (stop - start) // 2))
        def _(step):
            density = two(
                lambda group: low(wide(own[tile(group), :]) * wide(weighted[tile(group), :])), step
            )
            value = dot(left_b[...], low(dot(density, right_c[...])))
            field[tile(2 * step), :] = value[:, :LANES]
            field[tile(2 * step + 1), :] = value[:, LANES:]

    def strip(a, group):
        return pl.ds(pl.multiple_of(a * NG + group * SUB, SUB), SUB)

    def turn(unroll):
        @pl.loop(0, tiles // 2, unroll=unroll)
        def _(step):
            value = two(
                lambda group: low(
                    jnp.concatenate([field[strip(a, group), :] for a in range(HALF)], axis=0)
                ),
                step,
            )
            value = low(halved(dot(left_a[...], value)))
            value = low(wide(value) * two(lambda group: kern[tile(group), :], step))
            value = low(halved(dot(back_a[...], value)))
            value = dot(value, right_c[...])
            for side in range(2):
                for a in range(HALF):
                    field[strip(a, 2 * step + side), :] = value[
                        a * SUB : (a + 1) * SUB, side * LANES : (side + 1) * LANES
                    ]

    def fall(weighted, step):
        value = dot(left_b[...], two(lambda group: low(field[tile(group), :]), step))
        return [
            value[:, side * LANES : (side + 1) * LANES] * wide(weighted[tile(2 * step + side), :])
            for side in range(2)
        ]

    load_tables = pltpu.make_async_copy(tables_hbm, factors, load_sem.at[LOADS + 1])
    load_tri = pltpu.make_async_copy(tri_hbm, tri_line, load_sem.at[LOADS])

    for piece in range(LOADS):
        for half in range(2):
            load_orb(piece, half).start()

    def greet(i):
        pl.semaphore_signal(
            barrier, inc=1, device_id={"band": mate(i + 1)}, device_id_type=MESH
        )

    each(count, count - 1, lambda i: greet(count - 2 - i))

    load_tri.start()
    load_tables.start()

    fill = occ[0:1, :]
    for piece in range(LOADS):
        loaded_orb(piece).wait()

        @pl.loop(piece * HALF // LOADS, (piece + 1) * HALF // LOADS, unroll=2)
        def _(a):
            pair = jnp.concatenate(exchanged(plane(orb_line, a), plane(orb_line, a + HALF)), axis=0)
            cut = pl.ds(pl.multiple_of(a * NG, NG), NG)
            own[cut, :] = low(pair)
            own_w[cut, :] = low(pair * fill)


    load_tri.wait()

    @pl.loop(0, NG, unroll=2)
    def _(a):
        flat_t[pl.ds(pl.multiple_of(a * HALF, HALF), HALF), :] = low(plane(tri_line, a))

    load_tables.wait()
    pl.semaphore_wait(barrier, count - 1)
    for chunk in range(CHUNKS):
        orbital(chunk).start()
    to_sibling.start()

    trial_copy(1).start()

    def send_trial(step):
        relay_copy(step, me).start()
        trial_copy(step).start()

    each(count, 2 * (far - 1), lambda t: send_trial((far - t // 2) * 4 + t % 2))

    @pl.loop(0, tiles)
    def _(group):
        kern[tile(group), :] = screened_rows(group)

    rise(own_w, 0, tiles)
    turn(UNROLL)

    @pl.loop(0, tiles // 2, unroll=UNROLL)
    def _(step):
        for side, value in enumerate(fall(own_w, step)):
            acc[tile(2 * step + side), :] = value

    if far > 0:
        for low_bit in range(2):
            send_trial(4 + low_bit)
    to_sibling.wait_recv()
    rise(sibling, 0, tiles)
    turn(UNROLL)

    @pl.loop(0, tiles // 2, unroll=UNROLL)
    def _(step):
        for side, value in enumerate(fall(sibling, step)):
            acc[tile(2 * step + side), :] += value

    for chunk in range(CHUNKS - 1):
        orbital(chunk).wait_recv()
        rise(remote, chunk * tiles // CHUNKS, (chunk + 1) * tiles // CHUNKS)
    orbital(CHUNKS - 1).wait_recv()
    for step in range(2, min(count, 4)):
        trial_copy(step).start()
    rise(remote, tiles - tiles // CHUNKS, tiles)
    turn(LAST_UNROLL)

    @pl.loop(0, tiles // 2, unroll=UNROLL)
    def _(step):
        for side, value in enumerate(fall(remote, step)):
            group = 2 * step + side
            value = -FRACTION * (acc[tile(group), :] + value)
            for j in range(per_tile):
                a = group * per_tile + j
                first, second = exchanged(
                    value[j * NG : j * NG + HALF], value[j * NG + HALF : (j + 1) * NG]
                )
                flat_e[pl.ds(pl.multiple_of(a * HALF, HALF), HALF), :] = low(first)
                flat_e[pl.ds(pl.multiple_of((a + HALF) * HALF, HALF), HALF), :] = low(second)

    t_in[pl.ds(me, 1)] = tri_rows[pl.ds(me, 1)]
    e_in[pl.ds(me, 1)] = e_rows[pl.ds(me, 1)]
    def send_exchange(step):
        exchange_copy(step, me).start()

    near_steps(send_exchange)
    far_steps(4, send_exchange)

    def spread_out(src, dst, slot):
        dst[pl.ds(slot, slab, stride=count), :] = wide(src[slot])

    def take_exchange(step):
        peer = mate(step)
        exchange_copy(step, peer).wait_recv()
        spread_out(e_in, et, peer)

    @pl.loop(0, NG, unroll=2)
    def _(a):
        cut = pl.ds(pl.multiple_of(a * PLANE, PLANE), PLANE)
        rows = wide(flat_e[pl.ds(pl.multiple_of(a * HALF, HALF), HALF), :])
        exch_line[:, cut] = low(rows.reshape(1, PLANE))

    store_line = pltpu.make_async_copy(exch_line, line_out, out_sem.at[0])
    store_low = pltpu.make_async_copy(et_low, low_out, out_sem.at[1])
    store_line.start()
    def pass_on(t):
        two_slabs = pl.ds(0, 2)
        remote_copy(
            r_in.at[two_slabs], r_in.at[two_slabs], send_sem.at[TRIAL], r_recv.at[far - 1 - t], sib
        ).wait_recv()
        onward((far - t) * 4).start()
        onward((far - t) * 4 + 1).start()

    each(count, far, pass_on)
    several(tri_rows, t_in, TRIAL, count - 1).wait_recv()

    @pl.loop(0, count, unroll=4)
    def _(slot):
        spread_out(t_in, et, slot)

    @pl.loop(0, tiles, unroll=4)
    def _(group):
        tt[tile(group), :] = low(et[tile(group), :])

    spread_out(e_in, et, me)
    near_steps(take_exchange)
    far_steps(4, take_exchange)

    mine = [low(et[r * count : (r + 1) * count, :]) for r in range(slab)]
    for r in range(slab):
        et_low[r * count : (r + 1) * count, :] = mine[r]
    total = lax.dot_general(
        jnp.concatenate([tt[r * count : (r + 1) * count, :] for r in range(slab)], axis=1),
        jnp.concatenate(mine, axis=1),
        (((1,), (1,)), ((), ())),
        preferred_element_type=jnp.float32,
    )
    if spread > 1:
        rest = jnp.zeros((count, LANES - count), jnp.float32)
        total = jnp.concatenate([total, rest], axis=1)
        total = pltpu.roll(total, 0, 1, stride=count, stride_axis=0)
        total = jnp.sum(total.reshape(count // spread, spread, LANES), axis=1)
    part[...] = total
    parts[pl.ds(me, 1)] = total[None]

    def send_part(peer):
        @pl.when(peer != me)
        def _():
            part_copy(peer).start()

    each(count, count, send_part)
    store_low.start()
    own_sent.wait_send()
    several(tri_rows, t_in, TRIAL, count - 1).wait_send()
    if far > 0:
        several(r_in, t_in, ONWARD, 2 * far).wait_send()
    several(e_rows, e_in, EXCHANGE, count - 1).wait_send()
    store_line.wait()
    store_low.wait()
    several(parts, parts, PART, count - 1).wait()
    total_here[...] = jnp.sum(parts[...], axis=0)
    store_sum = pltpu.make_async_copy(total_here, summed, out_sem.at[2])
    store_sum.start()
    store_sum.wait()


def finish(count, exch_line, et_low, summed, exch_hbm, proj_hbm, proj, out_sem):
    pack = TILE // count
    spread = LANES // count
    groups = ROWS // TILE
    width = pack * LANES
    stores = []
    part = exch_line.shape[1] // PIECES
    for piece in range(PIECES):
        cut = pl.ds(piece * part, part)
        stores.append(
            pltpu.make_async_copy(
                exch_line.at[:, cut], exch_hbm.at[:, cut], out_sem.at[groups // 2 + piece]
            )
        )
        stores[-1].start()
    total = summed[...] / math.sqrt(ROWS * LANES)
    if spread > 1:
        total = jnp.broadcast_to(total[:, None, :], (count // spread, spread, LANES))
        total = jnp.where(own_lanes(count), total.reshape(count, LANES), 0.0)
    total = grown(total, count)
    mixing = low(total[:, :count])
    for group in range(groups):
        for r in range(0, pack, 2):
            row = (group * pack + r) * count
            at = (group * pack + r) * LANES
            sides = [et_low[row + k * count : row + (k + 1) * count, :] for k in range(2)]
            piece = dot(mixing, jnp.concatenate(sides, axis=1))
            proj[:, at : at + 2 * LANES] = low(piece * (-1.0 / math.sqrt(count)))
        if group % 2 == 1:
            cut = pl.ds((group - 1) * width, 2 * width)
            stores.append(
                pltpu.make_async_copy(proj.at[:, cut], proj_hbm.at[:, cut], out_sem.at[group // 2])
            )
            stores[-1].start()
    for store in stores:
        store.wait()


def local(orbitals, trial, occupations):
    count = lax.axis_size("band")
    cells = orbitals.shape[1]
    slab = ROWS // count
    rows = (ROWS, LANES)
    bf16, f32 = jnp.bfloat16, jnp.float32
    compact = (count // (LANES // count), LANES)
    dma = pltpu.SemaphoreType.DMA
    anywhere = pl.BlockSpec(memory_space=pl.ANY)
    vmem = pl.BlockSpec(memory_space=pltpu.VMEM)
    consts = tables()
    line, spread_low, summed = pl.pallas_call(
        functools.partial(body, count),
        out_shape=(
            jax.ShapeDtypeStruct((1, cells), bf16),
            jax.ShapeDtypeStruct(rows, bf16),
            jax.ShapeDtypeStruct(compact, f32),
        ),
        in_specs=[pl.BlockSpec(memory_space=pltpu.HBM)] * 3 + [vmem],
        out_specs=(anywhere, anywhere, anywhere),
        scratch_shapes=[
            pltpu.VMEM(consts.shape, bf16),
            pltpu.VMEM((1, cells), bf16),
            pltpu.VMEM((1, cells), bf16),
            pltpu.VMEM(rows, bf16),
            pltpu.VMEM(rows, bf16),
            pltpu.VMEM(rows, bf16),
            pltpu.VMEM(rows, bf16),
            pltpu.VMEM((count, slab, LANES), bf16),
            pltpu.VMEM(rows, f32),
            pltpu.VMEM(rows, f32),
            pltpu.VMEM(rows, f32),
            pltpu.VMEM((count, slab, LANES), bf16),
            pltpu.VMEM((count, slab, LANES), bf16),
            pltpu.VMEM((count, slab, LANES), bf16),
            pltpu.VMEM((count, slab, LANES), bf16),
            pltpu.VMEM(rows, bf16),
            pltpu.VMEM(rows, f32),
            pltpu.VMEM((1, cells), bf16),
            pltpu.VMEM(rows, bf16),
            pltpu.VMEM(compact, f32),
            pltpu.VMEM((count,) + compact, f32),
            pltpu.VMEM(compact, f32),
            dma((LOADS + 2,)),
            dma((5,)),
            dma((3,)),
            dma((CHUNKS,)),
            dma((max(count // 4 - 1, 1),)),
            dma((count - 1,)),
            dma((3,)),
        ],
        compiler_params=pltpu.CompilerParams(
            collective_id=1, has_side_effects=True, vmem_limit_bytes=VMEM_LIMIT
        ),
        name="exchange",
    )(
        *[pltpu.with_memory_space_constraint(x, pltpu.HBM) for x in (orbitals, trial, consts)],
        jnp.broadcast_to(occupations.astype(f32)[:, None], (8, LANES)),
    )
    return pl.pallas_call(
        functools.partial(finish, count),
        out_shape=(
            jax.ShapeDtypeStruct((1, cells), bf16),
            jax.ShapeDtypeStruct((count, cells // count), bf16),
        ),
        in_specs=[vmem, vmem, vmem],
        out_specs=(anywhere, anywhere),
        scratch_shapes=[
            pltpu.VMEM((count, cells // count), bf16),
            dma((ROWS // TILE // 2 + PIECES,)),
        ],
        compiler_params=pltpu.CompilerParams(vmem_limit_bytes=VMEM_LIMIT),
        name="finish",
    )(line, spread_low, summed)


def solution(mesh):
    return jax.shard_map(
        local,
        mesh=mesh,
        in_specs=(P(("spin", "band"), None), P(("spin", "band"), None), P(("spin", "band"))),
        out_specs=(P(("spin", "band"), None), P("spin", "band")),
        check_vma=False,
    )
```

```python
import functools
import math

import jax
import jax.numpy as jnp
import numpy as np
from jax import lax
from jax.experimental import pallas as pl
from jax.experimental.pallas import tpu as pltpu
from jax.sharding import PartitionSpec as P

NG = 64
FRACTION = 0.25
OMEGA = 1.0
LANES = 128
TILE = 256
CHUNKS = 4
UNROLL = 2
LAST_UNROLL = 2
VMEM_LIMIT = 30 << 20
WRITTEN_OUT = 32
PIECES = 1
LOADS = 2
OWN, TRIAL, PART, ONWARD, EXCHANGE = range(5)
MESH = pl.DeviceIdType.MESH

HALF = NG // 2
SUB = TILE // HALF
PLANE = NG * NG
ROWS = NG * NG * NG // LANES


def cas_table():
    index = np.arange(NG)
    phases = (index[:, None] * index[None, :] % NG).astype(np.float32) * np.float32(2.0 * math.pi / NG)
    return np.cos(phases) + np.sin(phases)


def tables():
    table = cas_table()
    order = np.concatenate([np.arange(0, NG, 2), np.arange(1, NG, 2)])
    eye = np.eye(TILE // NG, dtype=np.float32)
    sums = np.array([[1.0, 1.0], [1.0, -1.0]], np.float32)
    right_c = np.kron(np.eye(TILE // LANES, dtype=np.float32), np.kron(sums, table))
    left_b = np.kron(eye, table[order][:, order])
    halves = (table[0::2, :HALF], table[1::2, :HALF])
    rows = np.eye(TILE // HALF, dtype=np.float32)
    left_a = np.concatenate([np.kron(half, rows) for half in halves])
    back_a = np.concatenate([np.kron(half.T, rows) for half in halves])
    return jnp.asarray(np.concatenate([left_a, back_a, left_b, right_c])).astype(jnp.bfloat16)


def dot(left, right):
    return jnp.dot(left, right, preferred_element_type=jnp.float32)


def low(value):
    return value.astype(jnp.bfloat16)


def wide(value):
    return value.astype(jnp.float32)


def exchanged(first, second):
    lower = lax.broadcasted_iota(jnp.int32, first.shape, 1) < LANES // 2
    return (
        jnp.where(lower, first, pltpu.roll(second, LANES // 2, 1)),
        jnp.where(lower, pltpu.roll(first, LANES // 2, 1), second),
    )


def wavenum_sq(index):
    modes = wide(jnp.where(2 * index < NG, index, index - NG))
    wavenum = modes * (2.0 * math.pi / NG)
    return wavenum * wavenum


def screened_rows(group):
    shape = (TILE, LANES)
    row = lax.broadcasted_iota(jnp.int32, shape, 0)
    lane = lax.broadcasted_iota(jnp.int32, shape, 1)
    a = 2 * (row // SUB) + lane // NG
    place = group * SUB + row % SUB
    b = 2 * (place % HALF) + place // HALF
    norm_sq = wavenum_sq(a) + wavenum_sq(b) + wavenum_sq(lane % NG)
    bounded = jnp.where(norm_sq > 0, norm_sq, 1.0)
    screened = jnp.where(
        norm_sq > 0,
        4.0 * math.pi / bounded * (1.0 - jnp.exp(-bounded / (4.0 * OMEGA * OMEGA))),
        math.pi / (OMEGA * OMEGA),
    )
    return screened * (1.0 / NG**3)


def partner(me, step, count):
    total, bit = 0, 1
    while bit < count:
        total = total + bit * ((me // bit + step // bit) % 2)
        bit *= 2
    return total


def each(count, number, act):
    if count <= WRITTEN_OUT:
        for i in range(number):
            act(i)
    else:
        pl.loop(0, number)(act)


def grown(total, count):
    shift = LANES // 2
    while shift >= count:
        total = total + pltpu.roll(total, shift, 1)
        shift //= 2
    return total


def own_lanes(count):
    shape = (count, LANES)
    spread = LANES // count
    return (
        lax.broadcasted_iota(jnp.int32, shape, 0) % spread
        == lax.broadcasted_iota(jnp.int32, shape, 1) // count
    )


def body(
    count,
    orb_hbm, tri_hbm, tables_hbm, occ,
    line_out, low_out, summed,
    factors,
    orb_line, tri_line, own, own_w, sibling, remote, tri_rows, kern, field, acc,
    e_rows, t_in, r_in, e_in, tt, et, exch_line, et_low, part, parts, total_here,
    load_sem, send_sem, recv_sem, orb_recv, r_recv, e_recv, out_sem,
):
    me = lax.axis_index("band")
    flips = [bit * (1 - 2 * (me // bit % 2)) for bit in (1 << k for k in range(count.bit_length() - 1))]

    def mate(step):
        if isinstance(step, int):
            return me + sum(flip for k, flip in enumerate(flips) if step >> k & 1)
        return partner(me, step, count)

    barrier = pltpu.get_barrier_semaphore()
    slab = ROWS // count
    spread = LANES // count
    tiles = ROWS // TILE
    per_tile = TILE // NG
    depth = ROWS // CHUNKS
    span = HALF // LOADS * PLANE
    planes = max(count // 4, 1)
    sib = me + 1 - 2 * (me % 2)
    rem = (me + count - 1 + 2 * (me % 2)) % count
    left_a = factors.at[: 2 * TILE]
    back_a = factors.at[2 * TILE : 4 * TILE]
    left_b = factors.at[4 * TILE : 5 * TILE]
    right_c = factors.at[5 * TILE :]
    flat_t = tri_rows.reshape(ROWS, LANES)
    flat_e = e_rows.reshape(ROWS, LANES)

    far = planes - 1

    def far_steps(lows, act):
        def mixed(t):
            upper = t % far
            act((1 + upper) * 4 + (t // far + 2 * upper) % lows)

        each(count, lows * far, mixed)

    def far_first(lows, act):
        each(count, lows * far, lambda t: act((far - t // lows) * 4 + t % lows))

    def near_steps(act):
        for step in range(1, min(count, 4)):
            act(step)

    def load_orb(piece, half):
        cut = pl.ds((half * LOADS + piece) * span, span)
        return pltpu.make_async_copy(orb_hbm.at[:, cut], orb_line.at[:, cut], load_sem.at[piece])

    def loaded_orb(piece):
        cut = pl.ds(0, 2 * span)
        return pltpu.make_async_copy(orb_hbm.at[:, cut], orb_line.at[:, cut], load_sem.at[piece])

    def plane(ref, a):
        cut = pl.ds(pl.multiple_of(a * PLANE, PLANE), PLANE)
        return wide(ref[:, cut]).reshape(HALF, LANES)

    def remote_copy(src, dst, send, recv, peer):
        return pltpu.make_async_remote_copy(
            src_ref=src,
            dst_ref=dst,
            send_sem=send,
            recv_sem=recv,
            device_id={"band": peer},
            device_id_type=MESH,
        )

    def orbital(chunk):
        cut = pl.ds(chunk * depth, depth)
        return remote_copy(
            own_w.at[cut], remote.at[cut], send_sem.at[OWN], orb_recv.at[chunk], rem
        )

    to_sibling = remote_copy(own_w, sibling, send_sem.at[OWN], recv_sem.at[OWN], sib)
    own_sent = remote_copy(kern, field, send_sem.at[OWN], recv_sem.at[OWN], sib)

    def several(src, dst, kind, number):
        every = pl.ds(0, number)
        return remote_copy(
            src.at[every], dst.at[every], send_sem.at[kind], recv_sem.at[min(kind, PART)], sib
        )

    def trial_copy(step):
        peer = mate(step)
        return remote_copy(
            tri_rows.at[peer], t_in.at[me], send_sem.at[TRIAL], recv_sem.at[TRIAL], peer
        )

    def relay_copy(step, slot):
        return remote_copy(
            tri_rows.at[mate(step + 2)],
            r_in.at[slot],
            send_sem.at[TRIAL],
            r_recv.at[(step // 4 - 1) * 2 + step % 2],
            mate(step),
        )

    def onward(step):
        source = mate(step)
        return remote_copy(
            r_in.at[source], t_in.at[source], send_sem.at[ONWARD], recv_sem.at[TRIAL], mate(2)
        )

    def exchange_copy(step, slot):
        peer = mate(step)
        return remote_copy(
            e_rows.at[peer], e_in.at[slot], send_sem.at[EXCHANGE], e_recv.at[step - 1], peer
        )

    def part_copy(peer):
        return remote_copy(part, parts.at[me], send_sem.at[PART], recv_sem.at[PART], peer)

    def tile(group):
        return pl.ds(pl.multiple_of(group * TILE, TILE), TILE)

    def two(read, step):
        return jnp.concatenate([read(2 * step), read(2 * step + 1)], axis=1)

    def halved(value):
        lane = lax.broadcasted_iota(jnp.int32, (TILE, TILE), 1)
        return jnp.where(lane % LANES < LANES // 2, value[:TILE], value[TILE:])

    def rise(weighted, start, stop):
        @pl.loop(start // 2, stop // 2, unroll=min(UNROLL, (stop - start) // 2))
        def _(step):
            density = two(
                lambda group: low(wide(own[tile(group), :]) * wide(weighted[tile(group), :])), step
            )
            value = dot(left_b[...], low(dot(density, right_c[...])))
            field[tile(2 * step), :] = value[:, :LANES]
            field[tile(2 * step + 1), :] = value[:, LANES:]

    def strip(a, group):
        return pl.ds(pl.multiple_of(a * NG + group * SUB, SUB), SUB)

    def turn(unroll):
        @pl.loop(0, tiles // 2, unroll=unroll)
        def _(step):
            value = two(
                lambda group: low(
                    jnp.concatenate([field[strip(a, group), :] for a in range(HALF)], axis=0)
                ),
                step,
            )
            value = low(halved(dot(left_a[...], value)))
            value = low(wide(value) * two(lambda group: kern[tile(group), :], step))
            value = low(halved(dot(back_a[...], value)))
            value = dot(value, right_c[...])
            for side in range(2):
                for a in range(HALF):
                    field[strip(a, 2 * step + side), :] = value[
                        a * SUB : (a + 1) * SUB, side * LANES : (side + 1) * LANES
                    ]

    def fall(weighted, step):
        value = dot(left_b[...], two(lambda group: low(field[tile(group), :]), step))
        return [
            value[:, side * LANES : (side + 1) * LANES] * wide(weighted[tile(2 * step + side), :])
            for side in range(2)
        ]

    load_tables = pltpu.make_async_copy(tables_hbm, factors, load_sem.at[LOADS + 1])
    load_tri = pltpu.make_async_copy(tri_hbm, tri_line, load_sem.at[LOADS])

    def greet(i):
        pl.semaphore_signal(
            barrier, inc=1, device_id={"band": mate(i + 1)}, device_id_type=MESH
        )

    each(count, count - 1, lambda i: greet(count - 2 - i))

    for piece in range(LOADS):
        for half in range(2):
            load_orb(piece, half).start()
    load_tri.start()
    load_tables.start()

    fill = occ[0:1, :]
    for piece in range(LOADS):
        loaded_orb(piece).wait()

        @pl.loop(piece * HALF // LOADS, (piece + 1) * HALF // LOADS, unroll=2)
        def _(a):
            pair = jnp.concatenate(exchanged(plane(orb_line, a), plane(orb_line, a + HALF)), axis=0)
            cut = pl.ds(pl.multiple_of(a * NG, NG), NG)
            own[cut, :] = low(pair)
            own_w[cut, :] = low(pair * fill)


    load_tri.wait()

    @pl.loop(0, NG, unroll=2)
    def _(a):
        flat_t[pl.ds(pl.multiple_of(a * HALF, HALF), HALF), :] = low(plane(tri_line, a))

    load_tables.wait()
    pl.semaphore_wait(barrier, count - 1)
    for chunk in range(CHUNKS):
        orbital(chunk).start()
    to_sibling.start()

    trial_copy(1).start()

    def send_trial(step):
        relay_copy(step, me).start()
        trial_copy(step).start()

    if far > 0:
        for low_bit in range(2):
            send_trial(far * 4 + low_bit)

    @pl.loop(0, tiles)
    def _(group):
        kern[tile(group), :] = screened_rows(group)

    rise(own_w, 0, tiles)
    turn(UNROLL)

    @pl.loop(0, tiles // 2, unroll=UNROLL)
    def _(step):
        for side, value in enumerate(fall(own_w, step)):
            acc[tile(2 * step + side), :] = value

    each(count, 2 * (far - 1), lambda t: send_trial((far - 1 - t // 2) * 4 + t % 2))
    to_sibling.wait_recv()
    rise(sibling, 0, tiles)
    turn(UNROLL)

    @pl.loop(0, tiles // 2, unroll=UNROLL)
    def _(step):
        for side, value in enumerate(fall(sibling, step)):
            acc[tile(2 * step + side), :] += value

    for chunk in range(CHUNKS - 1):
        orbital(chunk).wait_recv()
        rise(remote, chunk * tiles // CHUNKS, (chunk + 1) * tiles // CHUNKS)
    orbital(CHUNKS - 1).wait_recv()
    for step in range(2, min(count, 4)):
        trial_copy(step).start()
    rise(remote, tiles - tiles // CHUNKS, tiles)
    turn(LAST_UNROLL)

    @pl.loop(0, tiles // 2, unroll=UNROLL)
    def _(step):
        for side, value in enumerate(fall(remote, step)):
            group = 2 * step + side
            value = -FRACTION * (acc[tile(group), :] + value)
            for j in range(per_tile):
                a = group * per_tile + j
                first, second = exchanged(
                    value[j * NG : j * NG + HALF], value[j * NG + HALF : (j + 1) * NG]
                )
                flat_e[pl.ds(pl.multiple_of(a * HALF, HALF), HALF), :] = low(first)
                flat_e[pl.ds(pl.multiple_of((a + HALF) * HALF, HALF), HALF), :] = low(second)

    t_in[pl.ds(me, 1)] = tri_rows[pl.ds(me, 1)]
    e_in[pl.ds(me, 1)] = e_rows[pl.ds(me, 1)]
    def send_exchange(step):
        exchange_copy(step, me).start()

    near_steps(send_exchange)
    far_steps(4, send_exchange)

    def spread_out(src, dst, slot):
        dst[pl.ds(slot, slab, stride=count), :] = wide(src[slot])

    def take_exchange(step):
        peer = mate(step)
        exchange_copy(step, peer).wait_recv()
        spread_out(e_in, et, peer)

    @pl.loop(0, NG, unroll=2)
    def _(a):
        cut = pl.ds(pl.multiple_of(a * PLANE, PLANE), PLANE)
        rows = wide(flat_e[pl.ds(pl.multiple_of(a * HALF, HALF), HALF), :])
        exch_line[:, cut] = low(rows.reshape(1, PLANE))

    store_line = pltpu.make_async_copy(exch_line, line_out, out_sem.at[0])
    store_low = pltpu.make_async_copy(et_low, low_out, out_sem.at[1])
    store_line.start()
    def pass_on(step):
        relay_copy(step, mate(step)).wait_recv()
        onward(step).start()

    far_steps(2, pass_on)
    several(tri_rows, t_in, TRIAL, count - 1).wait_recv()

    @pl.loop(0, count, unroll=4)
    def _(slot):
        spread_out(t_in, et, slot)

    @pl.loop(0, tiles, unroll=4)
    def _(group):
        tt[tile(group), :] = low(et[tile(group), :])

    spread_out(e_in, et, me)
    near_steps(take_exchange)
    far_steps(4, take_exchange)

    mine = [low(et[r * count : (r + 1) * count, :]) for r in range(slab)]
    total = lax.dot_general(
        jnp.concatenate([tt[r * count : (r + 1) * count, :] for r in range(slab)], axis=1),
        jnp.concatenate(mine, axis=1),
        (((1,), (1,)), ((), ())),
        preferred_element_type=jnp.float32,
    )
    if spread > 1:
        rest = jnp.zeros((count, LANES - count), jnp.float32)
        total = jnp.concatenate([total, rest], axis=1)
        total = pltpu.roll(total, 0, 1, stride=count, stride_axis=0)
        total = jnp.sum(total.reshape(count // spread, spread, LANES), axis=1)
    part[...] = total
    parts[pl.ds(me, 1)] = total[None]

    def send_part(peer):
        @pl.when(peer != me)
        def _():
            part_copy(peer).start()

    each(count, count, send_part)

    @pl.loop(0, tiles, unroll=4)
    def _(group):
        et_low[tile(group), :] = low(et[tile(group), :])

    store_low.start()
    own_sent.wait_send()
    several(tri_rows, t_in, TRIAL, count - 1).wait_send()
    if far > 0:
        several(r_in, t_in, ONWARD, 2 * far).wait_send()
    several(e_rows, e_in, EXCHANGE, count - 1).wait_send()
    store_line.wait()
    store_low.wait()
    several(parts, parts, PART, count - 1).wait()
    total_here[...] = jnp.sum(parts[...], axis=0)
    store_sum = pltpu.make_async_copy(total_here, summed, out_sem.at[2])
    store_sum.start()
    store_sum.wait()


def finish(count, exch_line, et_low, summed, exch_hbm, proj_hbm, proj, out_sem):
    pack = TILE // count
    spread = LANES // count
    groups = ROWS // TILE
    width = pack * LANES
    stores = []
    part = exch_line.shape[1] // PIECES
    for piece in range(PIECES):
        cut = pl.ds(piece * part, part)
        stores.append(
            pltpu.make_async_copy(
                exch_line.at[:, cut], exch_hbm.at[:, cut], out_sem.at[groups // 2 + piece]
            )
        )
        stores[-1].start()
    total = summed[...] / math.sqrt(ROWS * LANES)
    if spread > 1:
        total = jnp.broadcast_to(total[:, None, :], (count // spread, spread, LANES))
        total = jnp.where(own_lanes(count), total.reshape(count, LANES), 0.0)
    total = grown(total, count)
    mixing = low(total[:, :count])
    for group in range(groups):
        for r in range(0, pack, 2):
            row = (group * pack + r) * count
            at = (group * pack + r) * LANES
            sides = [et_low[row + k * count : row + (k + 1) * count, :] for k in range(2)]
            piece = dot(mixing, jnp.concatenate(sides, axis=1))
            proj[:, at : at + 2 * LANES] = low(piece * (-1.0 / math.sqrt(count)))
        if group % 2 == 1:
            cut = pl.ds((group - 1) * width, 2 * width)
            stores.append(
                pltpu.make_async_copy(proj.at[:, cut], proj_hbm.at[:, cut], out_sem.at[group // 2])
            )
            stores[-1].start()
    for store in stores:
        store.wait()


def local(orbitals, trial, occupations):
    count = lax.axis_size("band")
    cells = orbitals.shape[1]
    slab = ROWS // count
    rows = (ROWS, LANES)
    bf16, f32 = jnp.bfloat16, jnp.float32
    compact = (count // (LANES // count), LANES)
    dma = pltpu.SemaphoreType.DMA
    anywhere = pl.BlockSpec(memory_space=pl.ANY)
    vmem = pl.BlockSpec(memory_space=pltpu.VMEM)
    consts = tables()
    line, spread_low, summed = pl.pallas_call(
        functools.partial(body, count),
        out_shape=(
            jax.ShapeDtypeStruct((1, cells), bf16),
            jax.ShapeDtypeStruct(rows, bf16),
            jax.ShapeDtypeStruct(compact, f32),
        ),
        in_specs=[pl.BlockSpec(memory_space=pltpu.HBM)] * 3 + [vmem],
        out_specs=(anywhere, anywhere, anywhere),
        scratch_shapes=[
            pltpu.VMEM(consts.shape, bf16),
            pltpu.VMEM((1, cells), bf16),
            pltpu.VMEM((1, cells), bf16),
            pltpu.VMEM(rows, bf16),
            pltpu.VMEM(rows, bf16),
            pltpu.VMEM(rows, bf16),
            pltpu.VMEM(rows, bf16),
            pltpu.VMEM((count, slab, LANES), bf16),
            pltpu.VMEM(rows, f32),
            pltpu.VMEM(rows, f32),
            pltpu.VMEM(rows, f32),
            pltpu.VMEM((count, slab, LANES), bf16),
            pltpu.VMEM((count, slab, LANES), bf16),
            pltpu.VMEM((count, slab, LANES), bf16),
            pltpu.VMEM((count, slab, LANES), bf16),
            pltpu.VMEM(rows, bf16),
            pltpu.VMEM(rows, f32),
            pltpu.VMEM((1, cells), bf16),
            pltpu.VMEM(rows, bf16),
            pltpu.VMEM(compact, f32),
            pltpu.VMEM((count,) + compact, f32),
            pltpu.VMEM(compact, f32),
            dma((LOADS + 2,)),
            dma((5,)),
            dma((3,)),
            dma((CHUNKS,)),
            dma((max(2 * (count // 4 - 1), 1),)),
            dma((count - 1,)),
            dma((3,)),
        ],
        compiler_params=pltpu.CompilerParams(
            collective_id=1, has_side_effects=True, vmem_limit_bytes=VMEM_LIMIT
        ),
        name="exchange",
    )(
        *[pltpu.with_memory_space_constraint(x, pltpu.HBM) for x in (orbitals, trial, consts)],
        jnp.broadcast_to(occupations.astype(f32)[:, None], (8, LANES)),
    )
    return pl.pallas_call(
        functools.partial(finish, count),
        out_shape=(
            jax.ShapeDtypeStruct((1, cells), bf16),
            jax.ShapeDtypeStruct((count, cells // count), bf16),
        ),
        in_specs=[vmem, vmem, vmem],
        out_specs=(anywhere, anywhere),
        scratch_shapes=[
            pltpu.VMEM((count, cells // count), bf16),
            dma((ROWS // TILE // 2 + PIECES,)),
        ],
        compiler_params=pltpu.CompilerParams(vmem_limit_bytes=VMEM_LIMIT),
        name="finish",
    )(line, spread_low, summed)


def solution(mesh):
    return jax.shard_map(
        local,
        mesh=mesh,
        in_specs=(P(("spin", "band"), None), P(("spin", "band"), None), P(("spin", "band"))),
        out_specs=(P(("spin", "band"), None), P("spin", "band")),
        check_vma=False,
    )
```

```python
import functools
import math

import jax
import jax.numpy as jnp
import numpy as np
from jax import lax
from jax.experimental import pallas as pl
from jax.experimental.pallas import tpu as pltpu
from jax.sharding import PartitionSpec as P

NG = 64
FRACTION = 0.25
OMEGA = 1.0
LANES = 128
TILE = 256
CHUNKS = 4
UNROLL = 2
LAST_UNROLL = 2
VMEM_LIMIT = 30 << 20
WRITTEN_OUT = 32
PIECES = 1
LOADS = 2
OWN, TRIAL, PART, ONWARD, EXCHANGE = range(5)
MESH = pl.DeviceIdType.MESH

HALF = NG // 2
SUB = TILE // HALF
PLANE = NG * NG
ROWS = NG * NG * NG // LANES


def cas_table():
    index = np.arange(NG)
    phases = (index[:, None] * index[None, :] % NG).astype(np.float32) * np.float32(2.0 * math.pi / NG)
    return np.cos(phases) + np.sin(phases)


def tables():
    table = cas_table()
    order = np.concatenate([np.arange(0, NG, 2), np.arange(1, NG, 2)])
    eye = np.eye(TILE // NG, dtype=np.float32)
    sums = np.array([[1.0, 1.0], [1.0, -1.0]], np.float32)
    right_c = np.kron(np.eye(TILE // LANES, dtype=np.float32), np.kron(sums, table))
    left_b = np.kron(eye, table[order][:, order])
    halves = (table[0::2, :HALF], table[1::2, :HALF])
    rows = np.eye(TILE // HALF, dtype=np.float32)
    left_a = np.concatenate([np.kron(half, rows) for half in halves])
    back_a = np.concatenate([np.kron(half.T, rows) for half in halves])
    return jnp.asarray(np.concatenate([left_a, back_a, left_b, right_c])).astype(jnp.bfloat16)


def dot(left, right):
    return jnp.dot(left, right, preferred_element_type=jnp.float32)


def low(value):
    return value.astype(jnp.bfloat16)


def wide(value):
    return value.astype(jnp.float32)


def exchanged(first, second):
    lower = lax.broadcasted_iota(jnp.int32, first.shape, 1) < LANES // 2
    return (
        jnp.where(lower, first, pltpu.roll(second, LANES // 2, 1)),
        jnp.where(lower, pltpu.roll(first, LANES // 2, 1), second),
    )


def wavenum_sq(index):
    modes = wide(jnp.where(2 * index < NG, index, index - NG))
    wavenum = modes * (2.0 * math.pi / NG)
    return wavenum * wavenum


def screened_rows(group):
    shape = (TILE, LANES)
    row = lax.broadcasted_iota(jnp.int32, shape, 0)
    lane = lax.broadcasted_iota(jnp.int32, shape, 1)
    a = 2 * (row // SUB) + lane // NG
    place = group * SUB + row % SUB
    b = 2 * (place % HALF) + place // HALF
    norm_sq = wavenum_sq(a) + wavenum_sq(b) + wavenum_sq(lane % NG)
    bounded = jnp.where(norm_sq > 0, norm_sq, 1.0)
    screened = jnp.where(
        norm_sq > 0,
        4.0 * math.pi / bounded * (1.0 - jnp.exp(-bounded / (4.0 * OMEGA * OMEGA))),
        math.pi / (OMEGA * OMEGA),
    )
    return screened * (1.0 / NG**3)


def partner(me, step, count):
    total, bit = 0, 1
    while bit < count:
        total = total + bit * ((me // bit + step // bit) % 2)
        bit *= 2
    return total


def each(count, number, act):
    if count <= WRITTEN_OUT:
        for i in range(number):
            act(i)
    else:
        pl.loop(0, number)(act)


def grown(total, count):
    shift = LANES // 2
    while shift >= count:
        total = total + pltpu.roll(total, shift, 1)
        shift //= 2
    return total


def own_lanes(count):
    shape = (count, LANES)
    spread = LANES // count
    return (
        lax.broadcasted_iota(jnp.int32, shape, 0) % spread
        == lax.broadcasted_iota(jnp.int32, shape, 1) // count
    )


def body(
    count,
    orb_hbm, tri_hbm, tables_hbm, occ,
    line_out, low_out, summed,
    factors,
    orb_line, tri_line, own, own_w, sibling, remote, tri_rows, kern, field, acc,
    e_rows, t_in, r_in, e_in, tt, et, exch_line, et_low, part, parts, total_here,
    load_sem, send_sem, recv_sem, orb_recv, r_recv, e_recv, out_sem,
):
    me = lax.axis_index("band")
    flips = [bit * (1 - 2 * (me // bit % 2)) for bit in (1 << k for k in range(count.bit_length() - 1))]

    def mate(step):
        if isinstance(step, int):
            return me + sum(flip for k, flip in enumerate(flips) if step >> k & 1)
        return partner(me, step, count)

    barrier = pltpu.get_barrier_semaphore()
    slab = ROWS // count
    spread = LANES // count
    tiles = ROWS // TILE
    per_tile = TILE // NG
    depth = ROWS // CHUNKS
    span = HALF // LOADS * PLANE
    planes = max(count // 4, 1)
    sib = me + 1 - 2 * (me % 2)
    rem = (me + count - 1 + 2 * (me % 2)) % count
    left_a = factors.at[: 2 * TILE]
    back_a = factors.at[2 * TILE : 4 * TILE]
    left_b = factors.at[4 * TILE : 5 * TILE]
    right_c = factors.at[5 * TILE :]
    flat_t = tri_rows.reshape(ROWS, LANES)
    flat_e = e_rows.reshape(ROWS, LANES)

    far = planes - 1

    def far_steps(lows, act):
        def mixed(t):
            upper = t % far
            act((1 + upper) * 4 + (t // far + 2 * upper) % lows)

        each(count, lows * far, mixed)

    def far_first(lows, act):
        each(count, lows * far, lambda t: act((far - t // lows) * 4 + t % lows))

    def near_steps(act):
        for step in range(1, min(count, 4)):
            act(step)

    def load_orb(piece, half):
        cut = pl.ds((half * LOADS + piece) * span, span)
        return pltpu.make_async_copy(orb_hbm.at[:, cut], orb_line.at[:, cut], load_sem.at[piece])

    def loaded_orb(piece):
        cut = pl.ds(0, 2 * span)
        return pltpu.make_async_copy(orb_hbm.at[:, cut], orb_line.at[:, cut], load_sem.at[piece])

    def plane(ref, a):
        cut = pl.ds(pl.multiple_of(a * PLANE, PLANE), PLANE)
        return wide(ref[:, cut]).reshape(HALF, LANES)

    def remote_copy(src, dst, send, recv, peer):
        return pltpu.make_async_remote_copy(
            src_ref=src,
            dst_ref=dst,
            send_sem=send,
            recv_sem=recv,
            device_id={"band": peer},
            device_id_type=MESH,
        )

    def orbital(chunk):
        cut = pl.ds(chunk * depth, depth)
        return remote_copy(
            own_w.at[cut], remote.at[cut], send_sem.at[OWN], orb_recv.at[chunk], rem
        )

    to_sibling = remote_copy(own_w, sibling, send_sem.at[OWN], recv_sem.at[OWN], sib)
    own_sent = remote_copy(kern, field, send_sem.at[OWN], recv_sem.at[OWN], sib)

    def several(src, dst, kind, number):
        every = pl.ds(0, number)
        return remote_copy(
            src.at[every], dst.at[every], send_sem.at[kind], recv_sem.at[min(kind, PART)], sib
        )

    def trial_copy(step):
        peer = mate(step)
        return remote_copy(
            tri_rows.at[peer], t_in.at[me], send_sem.at[TRIAL], recv_sem.at[TRIAL], peer
        )

    def relay_copy(step, slot):
        return remote_copy(
            tri_rows.at[mate(step + 2)],
            r_in.at[slot],
            send_sem.at[TRIAL],
            r_recv.at[(step // 4 - 1) * 2 + step % 2],
            mate(step),
        )

    def onward(step):
        source = mate(step)
        return remote_copy(
            r_in.at[source], t_in.at[source], send_sem.at[ONWARD], recv_sem.at[TRIAL], mate(2)
        )

    def exchange_copy(step, slot):
        peer = mate(step)
        return remote_copy(
            e_rows.at[peer], e_in.at[slot], send_sem.at[EXCHANGE], e_recv.at[step - 1], peer
        )

    def part_copy(peer):
        return remote_copy(part, parts.at[me], send_sem.at[PART], recv_sem.at[PART], peer)

    def tile(group):
        return pl.ds(pl.multiple_of(group * TILE, TILE), TILE)

    def two(read, step):
        return jnp.concatenate([read(2 * step), read(2 * step + 1)], axis=1)

    def halved(value):
        lane = lax.broadcasted_iota(jnp.int32, (TILE, TILE), 1)
        return jnp.where(lane % LANES < LANES // 2, value[:TILE], value[TILE:])

    def rise(weighted, start, stop):
        @pl.loop(start // 2, stop // 2, unroll=min(UNROLL, (stop - start) // 2))
        def _(step):
            density = two(
                lambda group: low(wide(own[tile(group), :]) * wide(weighted[tile(group), :])), step
            )
            value = dot(left_b[...], low(dot(density, right_c[...])))
            field[tile(2 * step), :] = value[:, :LANES]
            field[tile(2 * step + 1), :] = value[:, LANES:]

    def strip(a, group):
        return pl.ds(pl.multiple_of(a * NG + group * SUB, SUB), SUB)

    def turn(unroll):
        @pl.loop(0, tiles // 2, unroll=unroll)
        def _(step):
            value = two(
                lambda group: low(
                    jnp.concatenate([field[strip(a, group), :] for a in range(HALF)], axis=0)
                ),
                step,
            )
            value = low(halved(dot(left_a[...], value)))
            value = low(wide(value) * two(lambda group: kern[tile(group), :], step))
            value = low(halved(dot(back_a[...], value)))
            value = dot(value, right_c[...])
            for side in range(2):
                for a in range(HALF):
                    field[strip(a, 2 * step + side), :] = value[
                        a * SUB : (a + 1) * SUB, side * LANES : (side + 1) * LANES
                    ]

    def fall(weighted, step):
        value = dot(left_b[...], two(lambda group: low(field[tile(group), :]), step))
        return [
            value[:, side * LANES : (side + 1) * LANES] * wide(weighted[tile(2 * step + side), :])
            for side in range(2)
        ]

    load_tables = pltpu.make_async_copy(tables_hbm, factors, load_sem.at[LOADS + 1])
    load_tri = pltpu.make_async_copy(tri_hbm, tri_line, load_sem.at[LOADS])

    def greet(i):
        pl.semaphore_signal(
            barrier, inc=1, device_id={"band": mate(i + 1)}, device_id_type=MESH
        )

    each(count, count - 1, lambda i: greet(count - 2 - i))

    for piece in range(LOADS):
        for half in range(2):
            load_orb(piece, half).start()
    load_tri.start()
    load_tables.start()

    fill = occ[0:1, :]
    for piece in range(LOADS):
        loaded_orb(piece).wait()

        @pl.loop(piece * HALF // LOADS, (piece + 1) * HALF // LOADS, unroll=2)
        def _(a):
            pair = jnp.concatenate(exchanged(plane(orb_line, a), plane(orb_line, a + HALF)), axis=0)
            cut = pl.ds(pl.multiple_of(a * NG, NG), NG)
            own[cut, :] = low(pair)
            own_w[cut, :] = low(pair * fill)


    load_tri.wait()

    @pl.loop(0, NG, unroll=2)
    def _(a):
        flat_t[pl.ds(pl.multiple_of(a * HALF, HALF), HALF), :] = low(plane(tri_line, a))

    load_tables.wait()
    pl.semaphore_wait(barrier, count - 1)
    for chunk in range(CHUNKS):
        orbital(chunk).start()
    to_sibling.start()

    trial_copy(1).start()

    def send_trial(step):
        relay_copy(step, me).start()
        trial_copy(step).start()

    each(count, 2 * (far - 1), lambda t: send_trial((far - t // 2) * 4 + t % 2))

    @pl.loop(0, tiles)
    def _(group):
        kern[tile(group), :] = screened_rows(group)

    rise(own_w, 0, tiles)
    turn(UNROLL)

    @pl.loop(0, tiles // 2, unroll=UNROLL)
    def _(step):
        for side, value in enumerate(fall(own_w, step)):
            acc[tile(2 * step + side), :] = value

    if far > 0:
        for low_bit in range(2):
            send_trial(4 + low_bit)
    to_sibling.wait_recv()
    rise(sibling, 0, tiles)
    turn(UNROLL)

    @pl.loop(0, tiles // 2, unroll=UNROLL)
    def _(step):
        for side, value in enumerate(fall(sibling, step)):
            acc[tile(2 * step + side), :] += value

    for chunk in range(CHUNKS - 1):
        orbital(chunk).wait_recv()
        rise(remote, chunk * tiles // CHUNKS, (chunk + 1) * tiles // CHUNKS)
    orbital(CHUNKS - 1).wait_recv()
    for step in range(2, min(count, 4)):
        trial_copy(step).start()
    rise(remote, tiles - tiles // CHUNKS, tiles)
    turn(LAST_UNROLL)

    @pl.loop(0, tiles // 2, unroll=UNROLL)
    def _(step):
        for side, value in enumerate(fall(remote, step)):
            group = 2 * step + side
            value = -FRACTION * (acc[tile(group), :] + value)
            for j in range(per_tile):
                a = group * per_tile + j
                first, second = exchanged(
                    value[j * NG : j * NG + HALF], value[j * NG + HALF : (j + 1) * NG]
                )
                flat_e[pl.ds(pl.multiple_of(a * HALF, HALF), HALF), :] = low(first)
                flat_e[pl.ds(pl.multiple_of((a + HALF) * HALF, HALF), HALF), :] = low(second)

    t_in[pl.ds(me, 1)] = tri_rows[pl.ds(me, 1)]
    e_in[pl.ds(me, 1)] = e_rows[pl.ds(me, 1)]
    def send_exchange(step):
        exchange_copy(step, me).start()

    near_steps(send_exchange)
    far_steps(4, send_exchange)

    def spread_out(src, dst, slot):
        dst[pl.ds(slot, slab, stride=count), :] = wide(src[slot])

    def take_exchange(step):
        peer = mate(step)
        exchange_copy(step, peer).wait_recv()
        spread_out(e_in, et, peer)

    @pl.loop(0, NG, unroll=2)
    def _(a):
        cut = pl.ds(pl.multiple_of(a * PLANE, PLANE), PLANE)
        rows = wide(flat_e[pl.ds(pl.multiple_of(a * HALF, HALF), HALF), :])
        exch_line[:, cut] = low(rows.reshape(1, PLANE))

    store_line = pltpu.make_async_copy(exch_line, line_out, out_sem.at[0])
    store_low = pltpu.make_async_copy(et_low, low_out, out_sem.at[1])
    store_line.start()
    def pass_on(step):
        relay_copy(step, mate(step)).wait_recv()
        onward(step).start()

    far_steps(2, pass_on)
    several(tri_rows, t_in, TRIAL, count - 1).wait_recv()

    @pl.loop(0, count, unroll=4)
    def _(slot):
        spread_out(t_in, et, slot)

    @pl.loop(0, tiles, unroll=4)
    def _(group):
        tt[tile(group), :] = low(et[tile(group), :])

    spread_out(e_in, et, me)
    near_steps(take_exchange)
    far_steps(4, take_exchange)

    mine = [low(et[r * count : (r + 1) * count, :]) for r in range(slab)]
    total = lax.dot_general(
        jnp.concatenate([tt[r * count : (r + 1) * count, :] for r in range(slab)], axis=1),
        jnp.concatenate(mine, axis=1),
        (((1,), (1,)), ((), ())),
        preferred_element_type=jnp.float32,
    )
    if spread > 1:
        rest = jnp.zeros((count, LANES - count), jnp.float32)
        total = jnp.concatenate([total, rest], axis=1)
        total = pltpu.roll(total, 0, 1, stride=count, stride_axis=0)
        total = jnp.sum(total.reshape(count // spread, spread, LANES), axis=1)
    part[...] = total
    parts[pl.ds(me, 1)] = total[None]

    def send_part(peer):
        @pl.when(peer != me)
        def _():
            part_copy(peer).start()

    each(count, count, send_part)

    @pl.loop(0, tiles, unroll=4)
    def _(group):
        et_low[tile(group), :] = low(et[tile(group), :])

    store_low.start()
    own_sent.wait_send()
    several(tri_rows, t_in, TRIAL, count - 1).wait_send()
    if far > 0:
        several(r_in, t_in, ONWARD, 2 * far).wait_send()
    several(e_rows, e_in, EXCHANGE, count - 1).wait_send()
    store_line.wait()
    store_low.wait()
    several(parts, parts, PART, count - 1).wait()
    total_here[...] = jnp.sum(parts[...], axis=0)
    store_sum = pltpu.make_async_copy(total_here, summed, out_sem.at[2])
    store_sum.start()
    store_sum.wait()


def finish(count, exch_line, et_low, summed, exch_hbm, proj_hbm, proj, out_sem):
    pack = TILE // count
    spread = LANES // count
    groups = ROWS // TILE
    width = pack * LANES
    stores = []
    part = exch_line.shape[1] // PIECES
    for piece in range(PIECES):
        cut = pl.ds(piece * part, part)
        stores.append(
            pltpu.make_async_copy(
                exch_line.at[:, cut], exch_hbm.at[:, cut], out_sem.at[groups // 2 + piece]
            )
        )
        stores[-1].start()
    total = summed[...] / math.sqrt(ROWS * LANES)
    if spread > 1:
        total = jnp.broadcast_to(total[:, None, :], (count // spread, spread, LANES))
        total = jnp.where(own_lanes(count), total.reshape(count, LANES), 0.0)
    total = grown(total, count)
    mixing = low(total[:, :count])
    for group in range(groups):
        for r in range(0, pack, 2):
            row = (group * pack + r) * count
            at = (group * pack + r) * LANES
            sides = [et_low[row + k * count : row + (k + 1) * count, :] for k in range(2)]
            piece = dot(mixing, jnp.concatenate(sides, axis=1))
            proj[:, at : at + 2 * LANES] = low(piece * (-1.0 / math.sqrt(count)))
        if group % 2 == 1:
            cut = pl.ds((group - 1) * width, 2 * width)
            stores.append(
                pltpu.make_async_copy(proj.at[:, cut], proj_hbm.at[:, cut], out_sem.at[group // 2])
            )
            stores[-1].start()
    for store in stores:
        store.wait()


def local(orbitals, trial, occupations):
    count = lax.axis_size("band")
    cells = orbitals.shape[1]
    slab = ROWS // count
    rows = (ROWS, LANES)
    bf16, f32 = jnp.bfloat16, jnp.float32
    compact = (count // (LANES // count), LANES)
    dma = pltpu.SemaphoreType.DMA
    anywhere = pl.BlockSpec(memory_space=pl.ANY)
    vmem = pl.BlockSpec(memory_space=pltpu.VMEM)
    consts = tables()
    line, spread_low, summed = pl.pallas_call(
        functools.partial(body, count),
        out_shape=(
            jax.ShapeDtypeStruct((1, cells), bf16),
            jax.ShapeDtypeStruct(rows, bf16),
            jax.ShapeDtypeStruct(compact, f32),
        ),
        in_specs=[pl.BlockSpec(memory_space=pltpu.HBM)] * 3 + [vmem],
        out_specs=(anywhere, anywhere, anywhere),
        scratch_shapes=[
            pltpu.VMEM(consts.shape, bf16),
            pltpu.VMEM((1, cells), bf16),
            pltpu.VMEM((1, cells), bf16),
            pltpu.VMEM(rows, bf16),
            pltpu.VMEM(rows, bf16),
            pltpu.VMEM(rows, bf16),
            pltpu.VMEM(rows, bf16),
            pltpu.VMEM((count, slab, LANES), bf16),
            pltpu.VMEM(rows, f32),
            pltpu.VMEM(rows, f32),
            pltpu.VMEM(rows, f32),
            pltpu.VMEM((count, slab, LANES), bf16),
            pltpu.VMEM((count, slab, LANES), bf16),
            pltpu.VMEM((count, slab, LANES), bf16),
            pltpu.VMEM((count, slab, LANES), bf16),
            pltpu.VMEM(rows, bf16),
            pltpu.VMEM(rows, f32),
            pltpu.VMEM((1, cells), bf16),
            pltpu.VMEM(rows, bf16),
            pltpu.VMEM(compact, f32),
            pltpu.VMEM((count,) + compact, f32),
            pltpu.VMEM(compact, f32),
            dma((LOADS + 2,)),
            dma((5,)),
            dma((3,)),
            dma((CHUNKS,)),
            dma((max(2 * (count // 4 - 1), 1),)),
            dma((count - 1,)),
            dma((3,)),
        ],
        compiler_params=pltpu.CompilerParams(
            collective_id=1, has_side_effects=True, vmem_limit_bytes=VMEM_LIMIT
        ),
        name="exchange",
    )(
        *[pltpu.with_memory_space_constraint(x, pltpu.HBM) for x in (orbitals, trial, consts)],
        jnp.broadcast_to(occupations.astype(f32)[:, None], (8, LANES)),
    )
    return pl.pallas_call(
        functools.partial(finish, count),
        out_shape=(
            jax.ShapeDtypeStruct((1, cells), bf16),
            jax.ShapeDtypeStruct((count, cells // count), bf16),
        ),
        in_specs=[vmem, vmem, vmem],
        out_specs=(anywhere, anywhere),
        scratch_shapes=[
            pltpu.VMEM((count, cells // count), bf16),
            dma((ROWS // TILE // 2 + PIECES,)),
        ],
        compiler_params=pltpu.CompilerParams(vmem_limit_bytes=VMEM_LIMIT),
        name="finish",
    )(line, spread_low, summed)


def solution(mesh):
    return jax.shard_map(
        local,
        mesh=mesh,
        in_specs=(P(("spin", "band"), None), P(("spin", "band"), None), P(("spin", "band"))),
        out_specs=(P(("spin", "band"), None), P("spin", "band")),
        check_vma=False,
    )
```
